128 devices in a mesh: zero: 32 (over z, x, core), model: 4 (over y).
Axes of the slice: x: 4, y: 4, z: 4, core: 2. Of those that a mesh axis runs over, the one named last changes fastest.
Arguments:
- w_query: bfloat16 [4096, 4096], P('zero', 'model'), may hold values from -0.1875 to 0.1875
- low_query: bfloat16 [4096, 16], P('zero'), may hold values from -0.09375 to 0.09375
- high_query: bfloat16 [16, 4096], P(None, 'model'), may hold values from -1.5 to 1.5
- w_key: bfloat16 [4096, 4096], P('zero', 'model'), may hold values from -0.1875 to 0.1875
- low_key: bfloat16 [4096, 16], P('zero'), may hold values from -0.09375 to 0.09375
- high_key: bfloat16 [16, 4096], P(None, 'model'), may hold values from -1.5 to 1.5
- w_value: bfloat16 [4096, 4096], P('zero', 'model'), may hold values from -0.1875 to 0.1875
- low_value: bfloat16 [4096, 16], P('zero'), may hold values from -0.09375 to 0.09375
- high_value: bfloat16 [16, 4096], P(None, 'model'), may hold values from -1.5 to 1.5
- norm_train: float32 [4096], P(('zero', 'model')), may hold values from 0.25 to 1.75
- norm_step: float32 [4096], P(('zero', 'model')), may hold values from -0.3 to 0.3
Outputs:
- serving_query: bfloat16 [4096, 4096], P(None, 'model')
- serving_key: bfloat16 [4096, 4096], P(None, 'model')
- serving_value: bfloat16 [4096, 4096], P(None, 'model')
- factor_query: float32 [4096], P('model')
- factor_key: float32 [4096], P('model')
- factor_value: float32 [4096], P('model')
- serve_norm: bfloat16 [4096], replicated
The draws below stay inside these ranges and needn't reach their ends.
All inputs are finite; a program needn't handle non-finite values. Where the reference program divides by a largest or mean magnitude, that divisor is 1e-20 or more.
Results may differ from the reference program's by a relative error of at most 0.001.
Values may be sent and summed in bfloat16 or wider, within the bound.
A program may use at most 128 MiB of HBM per device.

```python
import jax
import jax.numpy as jnp

D_MODEL = 4096
Q_DIM = 4096
KV_DIM = 4096
RANK = 16


def spiked(array, stream_key, source, target, parts, factor):
    def block_of(axis_at):
        return (jnp.arange(array.shape[axis_at]) // (array.shape[axis_at] // parts)).reshape((-1,) + (1,) * (array.ndim - 1 - axis_at))

    first = jax.random.permutation(stream_key, parts)[block_of(target)]
    other_side = (block_of(target) + parts // 2) % parts
    return jnp.where((block_of(source) == first) | (block_of(source) == other_side), factor * array, array)


def block_levels(key, dims, cuts, least, largest):
    loudness = 1.0
    for axis_at, parts in cuts:
        heights = jax.random.uniform(jax.random.fold_in(jax.random.fold_in(key, 6), axis_at), (parts,), jnp.float32, least / len(cuts), largest / len(cuts))
        loudness = loudness * jnp.repeat(jnp.exp(heights), dims[axis_at] // parts).reshape((-1,) + (1,) * (len(dims) - 1 - axis_at))
    return loudness


def noise(own_key, extent, width, bound, cuts=(), kind=jnp.bfloat16):
    array = width * jax.random.normal(own_key, extent, jnp.float32)
    if cuts:
        array = array * block_levels(own_key, extent, cuts, -0.22, 0.18)
    return jnp.clip(array, -bound, bound).astype(kind)


def bell_draw_with(rng, extent, scale, reach, pieces, heavy, held_as=jnp.bfloat16):
    drawn = scale * jax.random.normal(rng, extent, jnp.float32)
    if pieces:
        drawn = drawn * block_levels(rng, extent, pieces, -0.22, 0.18)
    return jnp.clip(spiked(drawn, jax.random.fold_in(rng, 3), *heavy), -reach, reach).astype(held_as)


def setup_inputs(seed: int = 0) -> dict:
    key_list = jax.random.split(jax.random.key(seed), 12)
    return {
        "w_query": bell_draw_with(key_list[0], (D_MODEL, Q_DIM), D_MODEL ** -0.5, 0.1875, ((0, 32), (1, 4)), (0, 1, 32, 2.75)),
        "low_query": noise(key_list[1], (D_MODEL, RANK), D_MODEL ** -0.5, 0.09375, ((0, 32),)),
        "high_query": noise(key_list[2], (RANK, Q_DIM), RANK ** -0.5, 1.5, ((1, 4),)),
        "w_key": bell_draw_with(key_list[3], (D_MODEL, KV_DIM), D_MODEL ** -0.5, 0.1875, ((0, 32), (1, 4)), (0, 1, 32, 2.75)),
        "low_key": noise(key_list[4], (D_MODEL, RANK), D_MODEL ** -0.5, 0.09375, ((0, 32),)),
        "high_key": noise(key_list[5], (RANK, KV_DIM), RANK ** -0.5, 1.5, ((1, 4),)),
        "w_value": bell_draw_with(key_list[6], (D_MODEL, KV_DIM), D_MODEL ** -0.5, 0.1875, ((0, 32), (1, 4)), (0, 1, 32, 2.75)),
        "low_value": noise(key_list[7], (D_MODEL, RANK), D_MODEL ** -0.5, 0.09375, ((0, 32),)),
        "high_value": noise(key_list[8], (RANK, KV_DIM), RANK ** -0.5, 1.5, ((1, 4),)),
        "norm_train": jnp.clip(1.0 + 0.15 * jax.random.normal(key_list[9], (D_MODEL,), jnp.float32), 0.25, 1.75),
        "norm_step": jnp.clip(jax.random.uniform(key_list[10], (D_MODEL,), jnp.float32, -0.3, 0.3) * block_levels(key_list[10], (D_MODEL,), ((0, 128),), -0.4, 0.0), -0.3, 0.3),
    }


mix_rate = 0.5


def reference(w_query, low_query, high_query, w_key, low_key, high_key, w_value, low_value, high_value, norm_train, norm_step):
    whole_query = w_query.astype(jnp.float32) + mix_rate * jnp.dot(low_query, high_query, preferred_element_type=jnp.float32)
    whole_key = w_key.astype(jnp.float32) + mix_rate * jnp.dot(low_key, high_key, preferred_element_type=jnp.float32)
    whole_value = w_value.astype(jnp.float32) + mix_rate * jnp.dot(low_value, high_value, preferred_element_type=jnp.float32)
    factor_query = jnp.sum(jnp.abs(whole_query), axis=0) / D_MODEL
    serving_query = (whole_query / factor_query).astype(jnp.bfloat16)
    factor_key = jnp.sum(jnp.abs(whole_key), axis=0) / D_MODEL
    serving_key = (whole_key / factor_key).astype(jnp.bfloat16)
    factor_value = jnp.sum(jnp.abs(whole_value), axis=0) / D_MODEL
    serving_value = (whole_value / factor_value).astype(jnp.bfloat16)
    serve_norm = (norm_train + norm_step).astype(jnp.bfloat16)
    return serving_query, serving_key, serving_value, factor_query, factor_key, factor_value, serve_norm
```

```python
import jax
import jax.numpy as jnp
from jax import lax
from jax.experimental import pallas as pl
from jax.experimental.pallas import tpu as pltpu
from jax.sharding import PartitionSpec as P

MESH = pl.DeviceIdType.MESH
D_MODEL = 4096
COLS = 1024
ROWS = 128
SUB = 32
SIDE = 4
AHEAD = 4

SLOTS = (
    (0, 0, 0, 0),
    (0, 0, 0, 1),
    (0, 0, 1, 0),
    (0, 0, 1, 1),
    (-1, 0, 0, 0),
    (0, -1, 1, 0),
    (0, 1, 1, 0),
    (0, -1, 1, 1),
    (0, 1, 1, 1),
    (0, 2, 1, 0),
    (0, 2, 1, 1),
    (-1, 0, 1, 0),
    (-1, -1, 1, 0),
    (-1, 1, 1, 0),
    (-1, 2, 1, 0),
)
N_SLOTS = len(SLOTS)


def gather_kernel(
    w_query, w_key, w_value, low_query, low_key, low_value, high_query, high_key, high_value, train, step,
    factors, norm, full,
    weights, lows, highs, whole, message, from_y, from_core, from_x, from_z,
    load_sem, small_send, small_recv, send_sem, recv_sem, pass_send, pass_recv, own_send, own_recv,
):
    zero, y = lax.axis_index("zero"), lax.axis_index("model")
    z, x, core = zero // 8, zero // 2 % 4, zero % 2
    partner = zero + 1 - 2 * core

    def index_of(z_at, x_at):
        return (z_at * 4 + x_at) * 2 + core

    loads = [
        pltpu.make_async_copy(src, dst, load_sem.at[k])
        for k, (src, dst) in enumerate(
            (
                (low_query, lows.at[0]), (low_key, lows.at[1]), (low_value, lows.at[2]),
                (high_query, highs.at[0]), (high_key, highs.at[1]), (high_value, highs.at[2]),
                (w_query, weights.at[0]), (w_key, weights.at[1]), (w_value, weights.at[2]),
            )
        )
    ]
    for load in loads:
        load.start()

    barrier = pltpu.get_barrier_semaphore()
    pl.semaphore_signal(barrier, inc=1, device_id=(partner, y), device_id_type=MESH)
    for k in range(1, SIDE):
        pl.semaphore_signal(barrier, inc=1, device_id=(index_of(z, (x + k) % 4), y), device_id_type=MESH)
        pl.semaphore_signal(barrier, inc=1, device_id=(index_of((z + k) % 4, x), y), device_id_type=MESH)
        pl.semaphore_signal(barrier, inc=1, device_id=(zero, (y + k) % 4), device_id_type=MESH)

    gain = train[...] + step[...]
    gain = pltpu.roll(jnp.concatenate([gain, jnp.zeros((1, 96), jnp.float32)], axis=1), 32 * y, 1)
    row = lax.broadcasted_iota(jnp.int32, (8, 128), 0)
    tile = jnp.where(row == x * 2 + core, jnp.broadcast_to(gain, (8, 128)), 0.0)
    from_y[pl.ds(y, 1)] = tile[None]
    pl.semaphore_wait(barrier, 10)

    def y_copy(k):
        return pltpu.make_async_remote_copy(
            src_ref=from_y.at[y], dst_ref=from_y.at[y],
            send_sem=small_send.at[k], recv_sem=small_recv.at[k],
            device_id=(zero, (y + k) % 4), device_id_type=MESH,
        )

    for k in range(1, SIDE):
        y_copy(k).start()

    for load in loads:
        load.wait()
    for m in range(3):
        product = lax.dot_general(
            lows[m], highs[m], (((0,), (0,)), ((), ())), preferred_element_type=jnp.float32
        )
        value = weights[m].astype(jnp.float32) + 0.5 * product
        whole[m] = value
        total = jnp.sum(jnp.abs(value), axis=0, keepdims=True)
        for j in range(8):
            message[m * 8 + j : m * 8 + j + 1, :] = total[:, j * 128 : (j + 1) * 128]
    for k in range(1, SIDE):
        y_copy(k).wait()
    message[24:32, :] = from_y[0] + from_y[1] + from_y[2] + from_y[3]

    core_copy = pltpu.make_async_remote_copy(
        src_ref=message, dst_ref=from_core,
        send_sem=small_send.at[0], recv_sem=small_recv.at[0],
        device_id=(partner, y), device_id_type=MESH,
    )
    core_copy.start()
    core_copy.wait()
    from_x[pl.ds(x, 1)] = (message[...] + from_core[...])[None]

    def x_copy(k):
        return pltpu.make_async_remote_copy(
            src_ref=from_x.at[x], dst_ref=from_x.at[x],
            send_sem=small_send.at[3 + k], recv_sem=small_recv.at[3 + k],
            device_id=(index_of(z, (x + k) % 4), y), device_id_type=MESH,
        )

    for k in range(1, SIDE):
        x_copy(k).start()
    for k in range(1, SIDE):
        x_copy(k).wait()
    from_z[pl.ds(z, 1)] = (from_x[0] + from_x[1] + from_x[2] + from_x[3])[None]

    def z_copy(k):
        return pltpu.make_async_remote_copy(
            src_ref=from_z.at[z], dst_ref=from_z.at[z],
            send_sem=small_send.at[6 + k], recv_sem=small_recv.at[6 + k],
            device_id=(index_of((z + k) % 4, x), y), device_id_type=MESH,
        )

    for k in range(1, SIDE):
        z_copy(k).start()
    for k in range(1, SIDE):
        z_copy(k).wait()
    total = from_z[0] + from_z[1] + from_z[2] + from_z[3]
    factor = total[:24] / D_MODEL
    factors[...] = factor
    inverse = 1.0 / factor
    for k in range(SIDE):
        norm[k * 8 : (k + 1) * 8, :] = from_z[k, 24:32, :].astype(jnp.bfloat16)

    own = pl.multiple_of(zero * ROWS, ROWS)
    for m in range(3):
        for j in range(8):
            scale = inverse[m * 8 + j : m * 8 + j + 1, :]
            full[m, pl.ds(own, ROWS), j * 128 : (j + 1) * 128] = (
                whole[m, :, j * 128 : (j + 1) * 128] * scale
            ).astype(jnp.bfloat16)

    def rows_of(link, slot, arriving):
        along, across, half, part = SLOTS[slot]
        axis, way = link // 2, 1 - 2 * (link % 2)
        along = (along - arriving) * way
        z_at = (z + axis * along + (1 - axis) * across + 8) % 4
        x_at = (x + (1 - axis) * along + axis * across + 8) % 4
        half = axis if half == 0 else 1 - axis
        part = link % 2 if part == 0 else 1 - link % 2
        return pl.multiple_of(index_of(z_at, x_at) * ROWS + half * 64 + part * SUB, SUB)

    def link_copy(link, slot, arriving=0):
        axis, way = link // 2, 1 - 2 * (link % 2)
        target = index_of((z + axis * way + 4) % 4, (x + (1 - axis) * way + 4) % 4)
        chunk = full.at[:, pl.ds(rows_of(link, slot, arriving), SUB), :]
        return pltpu.make_async_remote_copy(
            src_ref=chunk, dst_ref=chunk,
            send_sem=send_sem.at[slot * 4 + link], recv_sem=recv_sem.at[slot * 4 + link],
            device_id=(target, y), device_id_type=MESH,
        )

    def pass_copy(link, slot):
        chunk = full.at[:, pl.ds(rows_of(link, slot, 1), SUB), :]
        return pltpu.make_async_remote_copy(
            src_ref=chunk, dst_ref=chunk,
            send_sem=pass_send.at[slot * 4 + link], recv_sem=pass_recv.at[slot * 4 + link],
            device_id=(partner, y), device_id_type=MESH,
        )

    def each_link(body):
        def step_of(link, carry):
            body(link)
            return carry

        lax.fori_loop(0, 4, step_of, 0)

    for slot in range(AHEAD):
        each_link(lambda link: link_copy(link, slot).start())
    block = full.at[:, pl.ds(own, ROWS), :]
    own_copy = pltpu.make_async_remote_copy(
        src_ref=block, dst_ref=block, send_sem=own_send, recv_sem=own_recv,
        device_id=(partner, y), device_id_type=MESH,
    )
    own_copy.start()

    for slot in range(N_SLOTS):

        def arrive(link):
            link_copy(link, slot, 1).wait_recv()
            pass_copy(link, slot).start()

        each_link(arrive)
        if slot + AHEAD < N_SLOTS:
            each_link(lambda link: link_copy(link, slot + AHEAD).start())

    for slot in range(N_SLOTS):

        def finish(link):
            link_copy(link, slot).wait_send()
            pass_copy(link, slot).wait()

        each_link(finish)
    own_copy.wait()


def write_kernel(factors, norm, full, query, key, value, f_query, f_key, f_value, norm_out, sem):
    cuts = 4
    step = D_MODEL // cuts
    copies = [
        pltpu.make_async_copy(
            full.at[m, pl.ds(c * step, step), :], out.at[pl.ds(c * step, step), :], sem.at[m * cuts + c]
        )
        for m, out in enumerate((query, key, value))
        for c in range(cuts)
    ]
    for copy in copies:
        copy.start()
    for m, out in enumerate((f_query, f_key, f_value)):
        out[...] = factors[m * 8 : (m + 1) * 8, :]
    norm_out[...] = norm[...]
    for copy in copies:
        copy.wait()


def per_device(wq, lq, hq, wk, lk, hk, wv, lv, hv, train, step):
    any_spec = pl.BlockSpec(memory_space=pl.ANY)
    vmem = pl.BlockSpec(memory_space=pltpu.VMEM)
    f32, bf16 = jnp.float32, jnp.bfloat16
    hbm = [
        pltpu.with_memory_space_constraint(a, pltpu.HBM)
        for a in (wq, wk, wv, lq.T, lk.T, lv.T, hq, hk, hv, train.reshape(1, 32), step.reshape(1, 32))
    ]
    factors, norm, full = pl.pallas_call(
        gather_kernel,
        out_shape=(
            jax.ShapeDtypeStruct((24, 128), f32),
            jax.ShapeDtypeStruct((32, 128), bf16),
            pltpu.VMEM((3, D_MODEL, COLS), bf16),
        ),
        in_specs=[any_spec] * 9 + [vmem] * 2,
        out_specs=(vmem, vmem, vmem),
        scratch_shapes=[
            pltpu.VMEM((3, ROWS, COLS), bf16),
            pltpu.VMEM((3, 16, ROWS), bf16),
            pltpu.VMEM((3, 16, COLS), bf16),
            pltpu.VMEM((3, ROWS, COLS), f32),
            pltpu.VMEM((32, 128), f32),
            pltpu.VMEM((4, 8, 128), f32),
            pltpu.VMEM((32, 128), f32),
            pltpu.VMEM((4, 32, 128), f32),
            pltpu.VMEM((4, 32, 128), f32),
            pltpu.SemaphoreType.DMA((9,)),
            pltpu.SemaphoreType.DMA((10,)),
            pltpu.SemaphoreType.DMA((10,)),
            pltpu.SemaphoreType.DMA((N_SLOTS * 4,)),
            pltpu.SemaphoreType.DMA((N_SLOTS * 4,)),
            pltpu.SemaphoreType.DMA((N_SLOTS * 4,)),
            pltpu.SemaphoreType.DMA((N_SLOTS * 4,)),
            pltpu.SemaphoreType.DMA,
            pltpu.SemaphoreType.DMA,
        ],
        compiler_params=pltpu.CompilerParams(
            collective_id=0, has_side_effects=True, vmem_limit_bytes=16 * 1024 * 1024
        ),
    )(*hbm)
    query, key, value, f_query, f_key, f_value, norm = pl.pallas_call(
        write_kernel,
        out_shape=(
            jax.ShapeDtypeStruct((D_MODEL, COLS), bf16),
            jax.ShapeDtypeStruct((D_MODEL, COLS), bf16),
            jax.ShapeDtypeStruct((D_MODEL, COLS), bf16),
            jax.ShapeDtypeStruct((8, 128), f32),
            jax.ShapeDtypeStruct((8, 128), f32),
            jax.ShapeDtypeStruct((8, 128), f32),
            jax.ShapeDtypeStruct((32, 128), bf16),
        ),
        in_specs=[vmem] * 3,
        out_specs=[any_spec] * 3 + [vmem] * 4,
        scratch_shapes=[pltpu.SemaphoreType.DMA((12,))],
        compiler_params=pltpu.CompilerParams(vmem_limit_bytes=16 * 1024 * 1024),
    )(factors, norm, full)
    return (
        query, key, value,
        f_query.reshape(COLS), f_key.reshape(COLS), f_value.reshape(COLS), norm.reshape(D_MODEL),
    )


def solution(mesh):
    return jax.shard_map(
        per_device,
        mesh=mesh,
        in_specs=(
            P("zero", "model"), P("zero", None), P(None, "model"),
            P("zero", "model"), P("zero", None), P(None, "model"),
            P("zero", "model"), P("zero", None), P(None, "model"),
            P(("zero", "model")), P(("zero", "model")),
        ),
        out_specs=(
            P(None, "model"), P(None, "model"), P(None, "model"),
            P("model"), P("model"), P("model"), P(),
        ),
        check_vma=False,
    )
```

```python
import jax
import jax.numpy as jnp
from jax import lax
from jax.experimental import pallas as pl
from jax.experimental.pallas import tpu as pltpu
from jax.sharding import PartitionSpec as P

MESH = pl.DeviceIdType.MESH
D_MODEL = 4096
COLS = 1024
ROWS = 128
SUB = 32
SIDE = 4
GATHER_LIMIT = 16
WRITE_LIMIT = 18

MESSAGES = (
    (0, 0, 0, 2),
    (0, 0, 1, 2),
    (-1, 0, 0, 1),
    (0, -1, 1, 2),
    (0, 1, 1, 2),
    (0, 2, 1, 2),
    (-1, 0, 1, 1),
    (-1, -1, 1, 1),
    (-1, 1, 1, 1),
    (-1, 2, 1, 1),
)
N_MESSAGES = len(MESSAGES)


def scaled(low_rows, mixes, inverse, rows, start, source, store):
    low = low_rows[pl.ds(start, rows), :]
    for m in range(3):
        for pair in range(4):
            cols = slice(pair * 256, pair * 256 + 256)
            product = jnp.dot(low, mixes[m, :, cols], preferred_element_type=jnp.float32)
            for j in range(2):
                at = pair * 256 + j * 128
                row = m * 8 + pair * 2 + j
                whole = source[m, pl.ds(start, rows), at : at + 128].astype(jnp.float32) + product[:, j * 128 : j * 128 + 128]
                store(m, at, (whole * inverse[row : row + 1, :]).astype(jnp.bfloat16))


def gather_kernel(
    w_query, w_key, w_value, low_query, low_key, low_value, high_query, high_key, high_value, train, step,
    factors, inverse, norm, low_rows, mixes, full,
    lows, highs, message, from_y, from_core, from_first, from_second,
    load_sem, small_send, small_recv, send_sem, recv_sem, pass_send, pass_recv, own_send, own_recv,
):
    zero, y = lax.axis_index("zero"), lax.axis_index("model")
    z, x, core = zero // 8, zero // 2 % 4, zero % 2
    partner = zero + 1 - 2 * core
    own = pl.multiple_of(zero * ROWS, ROWS)
    first = x + core * (z - x)
    second = z + core * (x - z)

    def index_of(z_at, x_at, core_at):
        return (z_at * 4 + x_at) * 2 + core_at

    def peer(axis, k):
        return index_of((z + axis * k) % 4, (x + (1 - axis) * k) % 4, core)

    def remote(src, dst, sems, at, target, y_at):
        return pltpu.make_async_remote_copy(
            src_ref=src, dst_ref=dst, send_sem=sems[0].at[at], recv_sem=sems[1].at[at],
            device_id=(target, y_at), device_id_type=MESH,
        )

    small = (small_send, small_recv)
    place = second * 4 + first
    loads = [
        pltpu.make_async_copy(src, dst, load_sem.at[k])
        for k, (src, dst) in enumerate(
            (
                (w_query, full.at[0, pl.ds(own, ROWS), :]),
                (w_key, full.at[1, pl.ds(own, ROWS), :]),
                (w_value, full.at[2, pl.ds(own, ROWS), :]),
                (low_query, lows.at[core, place, pl.ds(0, 16), :]),
                (low_key, lows.at[core, place, pl.ds(16, 16), :]),
                (low_value, lows.at[core, place, pl.ds(32, 16), :]),
                (high_query, highs.at[0]), (high_key, highs.at[1]), (high_value, highs.at[2]),
            )
        )
    ]
    for load in loads:
        load.start()

    barrier = pltpu.get_barrier_semaphore()
    pl.semaphore_signal(barrier, inc=1, device_id=(partner, y), device_id_type=MESH)
    for k in range(1, SIDE):
        pl.semaphore_signal(barrier, inc=1, device_id=(peer(0, k), y), device_id_type=MESH)
        pl.semaphore_signal(barrier, inc=1, device_id=(peer(1, k), y), device_id_type=MESH)
        pl.semaphore_signal(barrier, inc=1, device_id=(zero, (y + k) % 4), device_id_type=MESH)

    gain = train[...] + step[...]
    gain = pltpu.roll(jnp.concatenate([gain, jnp.zeros((1, 96), jnp.float32)], axis=1), 32 * y, 1)
    row = lax.broadcasted_iota(jnp.int32, (8, 128), 0)
    tile = jnp.where(row == x * 2 + core, jnp.broadcast_to(gain, (8, 128)), 0.0)
    from_y[pl.ds(y, 1)] = tile[None]
    for load in loads[:3]:
        load.wait()
    pl.semaphore_wait(barrier, 10)

    def rows_of(link, at, arriving, core_at):
        along, across, half, parts = MESSAGES[at]
        axis, way = link // 2, 1 - 2 * (link % 2)
        along = (along - arriving) * way
        z_at = (z + axis * along + (1 - axis) * across + 8) % 4
        x_at = (x + (1 - axis) * along + axis * across + 8) % 4
        half = axis if half == 0 else 1 - axis
        part = link % 2 if parts == 1 else 0
        return pl.multiple_of(index_of(z_at, x_at, core_at) * ROWS + half * 64 + part * SUB, SUB)

    def chunk_of(link, at, arriving, core_at):
        return full.at[:, pl.ds(rows_of(link, at, arriving, core_at), MESSAGES[at][3] * SUB), :]

    def link_copy(link, at, arriving=0):
        axis, way = link // 2, 1 - 2 * (link % 2)
        chunk = chunk_of(link, at, arriving, core)
        target = index_of((z + axis * way + 4) % 4, (x + (1 - axis) * way + 4) % 4, core)
        return remote(chunk, chunk, (send_sem, recv_sem), at * 4 + link, target, y)

    def pass_copy(link, at, arriving_from=None):
        chunk = chunk_of(link, at, 1, core)
        return remote(chunk, chunk, (pass_send, pass_recv), at * 4 + link, partner, y)

    def each_link(body, count=4):
        def step_of(link, carry):
            body(link)
            return carry

        lax.fori_loop(0, count, step_of, 0)

    def send(at):
        each_link(lambda link: link_copy(link, at).start())

    def arrive(at):
        def body(link):
            link_copy(link, at, 1).wait_recv()
            pass_copy(link, at).start()

        each_link(body)

    send(0)
    block = full.at[:, pl.ds(own, ROWS), :]
    own_copy = pltpu.make_async_remote_copy(
        src_ref=block, dst_ref=block, send_sem=own_send, recv_sem=own_recv,
        device_id=(partner, y), device_id_type=MESH,
    )
    own_copy.start()
    y_copies = [
        remote(from_y.at[y], from_y.at[y], small, k, zero, (y + k) % 4) for k in range(1, SIDE)
    ]
    for copy in y_copies:
        copy.start()

    for load in loads[3:]:
        load.wait()
    low_own = lows.at[core, place]
    low_first = [remote(low_own, low_own, small, 10 + k, peer(core, k), y) for k in range(1, SIDE)]
    for copy in low_first:
        copy.start()
    send(1)
    for m in range(3):
        product = lax.dot_general(
            low_own[16 * m : 16 * m + 16, :], highs[m], (((0,), (0,)), ((), ())),
            preferred_element_type=jnp.float32,
        )
        value = full[m, pl.ds(own, ROWS), :].astype(jnp.float32) + 0.5 * product
        total = jnp.sum(jnp.abs(value), axis=0, keepdims=True)
        for j in range(8):
            message[m * 8 + j : m * 8 + j + 1, :] = total[:, j * 128 : (j + 1) * 128]
        mixes[m] = jnp.zeros((128, COLS), jnp.bfloat16)
        mixes[m, 16 * m : 16 * m + 16, :] = (0.5 * highs[m].astype(jnp.float32)).astype(jnp.bfloat16)
    for copy in y_copies:
        copy.wait()
    message[24:32, :] = from_y[0] + from_y[1] + from_y[2] + from_y[3]

    core_copy = remote(message, from_core, small, 0, partner, y)
    core_copy.start()
    core_copy.wait()
    share = 1 - core
    mine = pl.ds(pl.multiple_of(share * 16, 16), 16)
    from_first[pl.ds(first, 1)] = (message[mine, :] + from_core[mine, :])[None]
    first_copies = [
        remote(from_first.at[first], from_first.at[first], small, 3 + k, peer(core, k), y)
        for k in range(1, SIDE)
    ]
    for copy in first_copies:
        copy.start()

    arrive(0)
    send(2)
    send(3)
    for copy in first_copies + low_first:
        copy.wait()
    from_second[pl.ds(share, 1), pl.ds(second, 1)] = (
        from_first[0] + from_first[1] + from_first[2] + from_first[3]
    )[None, None]
    own_sum = from_second.at[share, second]
    second_copies = [remote(own_sum, own_sum, small, 6 + k, peer(1 - core, k), y) for k in range(1, SIDE)]
    low_line = lows.at[core, pl.ds(pl.multiple_of(second * 4, 4), 4)]
    second_copies += [remote(low_line, low_line, small, 13 + k, peer(1 - core, k), y) for k in range(1, SIDE)]
    for copy in second_copies:
        copy.start()

    arrive(1)
    send(4)
    for copy in second_copies:
        copy.wait()
    last_copies = [
        remote(from_second.at[share], from_second.at[share], small, 10, partner, y),
        remote(lows.at[core], lows.at[core], small, 17, partner, y),
    ]
    for copy in last_copies:
        copy.start()
    for copy in last_copies:
        copy.wait()
    sums = [from_second[h, 0] + from_second[h, 1] + from_second[h, 2] + from_second[h, 3] for h in range(2)]
    factor = jnp.concatenate([sums[0], sums[1][:8]], axis=0) / D_MODEL
    factors[...] = factor
    inverse[...] = 1.0 / factor
    for k in range(SIDE):
        norm[k * 8 : (k + 1) * 8, :] = from_second[1, k, 8:16, :].astype(jnp.bfloat16)

    arrive(2)
    send(5)
    lane = lax.broadcasted_iota(jnp.int32, (48, 128), 1)
    unit = jnp.where(lax.broadcasted_iota(jnp.int32, (48, 128), 0) == lane, 1.0, 0.0).astype(jnp.bfloat16)

    def turn(k, carry):
        core_at, major, minor = k // 16, k // 4 % 4, k % 4
        z_at = major + core_at * (minor - major)
        x_at = minor + core_at * (major - minor)
        start = pl.multiple_of(index_of(z_at, x_at, core_at) * ROWS, ROWS)
        turned = lax.dot_general(
            lows[core_at, k % 16], unit, (((0,), (0,)), ((), ())), preferred_element_type=jnp.float32
        )
        low_rows[pl.ds(start, ROWS), :] = turned.astype(jnp.bfloat16)
        return carry

    lax.fori_loop(0, 32, turn, 0)

    scale = inverse[...]

    def scale_rows(start):
        def store(m, at, value):
            full[m, pl.ds(start, 64), at : at + 128] = value

        scaled(low_rows, mixes, scale, 64, start, full, store)

    def scale_passed(at):
        def body(link):
            pass_copy(link, at).wait_recv()
            scale_rows(pl.multiple_of(rows_of(link, at, 1, 1 - core), 64))

        each_link(body)

    own_copy.wait_recv()
    each_link(lambda half: scale_rows(pl.multiple_of(partner * ROWS + half * 64, 64)), 2)
    scale_passed(0)
    arrive(3)
    send(6)
    send(7)
    scale_passed(1)

    def both_parts(axis):
        pass_copy(2 * axis, 2).wait_recv()
        pass_copy(2 * axis + 1, 2).wait_recv()
        scale_rows(pl.multiple_of(rows_of(2 * axis, 2, 1, 1 - core), 64))

    each_link(both_parts, 2)
    arrive(4)
    send(8)
    scale_passed(3)
    arrive(5)
    send(9)
    scale_passed(4)
    arrive(6)
    scale_passed(5)
    arrive(7)
    arrive(8)
    arrive(9)
    for at in range(N_MESSAGES):

        def finish(link):
            link_copy(link, at).wait_send()
            pass_copy(link, at).wait_send()
            if at > 5:
                pass_copy(link, at).wait_recv()

        each_link(finish)
    own_copy.wait_send()


def write_kernel(
    factors, inverse, norm, low_rows, mixes, full,
    query, key, value, f_query, f_key, f_value, norm_out, mine, late, sem,
):
    zero = lax.axis_index("zero")
    z, x, core = zero // 8, zero // 2 % 4, zero % 2
    outs = (query, key, value)

    def index_of(z_at, x_at, core_at):
        return (z_at * 4 + x_at) * 2 + core_at

    def ready_start(k):
        half, far, near = k // 12, k // 4 % 3, k % 4
        far = far + 3
        z_at = (z + (1 - half) * far + half * near) % 4
        x_at = (x + half * far + (1 - half) * near) % 4
        return pl.multiple_of(index_of(z_at, x_at, 1 - core) * ROWS + half * 64, 64)

    def late_start(k):
        half, near = k // 4, k % 4
        z_at = (z + (1 - half) * 2 + half * near) % 4
        x_at = (x + half * 2 + (1 - half) * near) % 4
        return pl.multiple_of(index_of(z_at, x_at, 1 - core) * ROWS + half * 64, 64)

    def mine_start(k):
        return pl.multiple_of((k * 2 + core) * ROWS, ROWS)

    def ready_copy(k, m):
        rows = pl.ds(ready_start(k), 64)
        return pltpu.make_async_copy(full.at[m, rows, :], outs[m].at[rows, :], sem.at[k * 3 + m])

    def mine_copy(k, m):
        return pltpu.make_async_copy(mine.at[k, m], outs[m].at[pl.ds(mine_start(k), ROWS), :], sem.at[72 + k * 3 + m])

    def late_copy(k, m):
        return pltpu.make_async_copy(late.at[k, m], outs[m].at[pl.ds(late_start(k), 64), :], sem.at[120 + k * 3 + m])

    def each(count, body):
        def step_of(k, carry):
            body(k)
            return carry

        lax.fori_loop(0, count, step_of, 0)

    def start_all(copy):
        def body(k):
            for m in range(3):
                copy(k, m).start()

        return body

    def wait_all(copy):
        def body(k):
            for m in range(3):
                copy(k, m).wait()

        return body

    each(24, start_all(ready_copy))
    for m, out in enumerate((f_query, f_key, f_value)):
        out[...] = factors[m * 8 : (m + 1) * 8, :]
    norm_out[...] = norm[...]
    scale = inverse[...]

    def scale_mine(k):
        def store(m, at, value):
            mine[k, m, :, at : at + 128] = value

        scaled(low_rows, mixes, scale, ROWS, mine_start(k), full, store)
        start_all(mine_copy)(k)

    def scale_late(k):
        def store(m, at, value):
            late[k, m, :, at : at + 128] = value

        scaled(low_rows, mixes, scale, 64, late_start(k), full, store)
        start_all(late_copy)(k)

    each(16, scale_mine)
    each(8, scale_late)
    each(24, wait_all(ready_copy))
    each(16, wait_all(mine_copy))
    each(8, wait_all(late_copy))


def per_device(wq, lq, hq, wk, lk, hk, wv, lv, hv, train, step):
    any_spec = pl.BlockSpec(memory_space=pl.ANY)
    vmem = pl.BlockSpec(memory_space=pltpu.VMEM)
    f32, bf16 = jnp.float32, jnp.bfloat16
    hbm = [
        pltpu.with_memory_space_constraint(a, pltpu.HBM)
        for a in (wq, wk, wv, lq.T, lk.T, lv.T, hq, hk, hv, train.reshape(1, 32), step.reshape(1, 32))
    ]
    state = pl.pallas_call(
        gather_kernel,
        out_shape=(
            jax.ShapeDtypeStruct((24, 128), f32),
            jax.ShapeDtypeStruct((24, 128), f32),
            jax.ShapeDtypeStruct((32, 128), bf16),
            pltpu.VMEM((D_MODEL, 128), bf16),
            pltpu.VMEM((3, 128, COLS), bf16),
            pltpu.VMEM((3, D_MODEL, COLS), bf16),
        ),
        in_specs=[any_spec] * 9 + [vmem] * 2,
        out_specs=(vmem,) * 6,
        scratch_shapes=[
            pltpu.VMEM((2, 16, 48, 128), bf16),
            pltpu.VMEM((3, 16, COLS), bf16),
            pltpu.VMEM((32, 128), f32),
            pltpu.VMEM((4, 8, 128), f32),
            pltpu.VMEM((32, 128), f32),
            pltpu.VMEM((4, 16, 128), f32),
            pltpu.VMEM((2, 4, 16, 128), f32),
            pltpu.SemaphoreType.DMA((9,)),
            pltpu.SemaphoreType.DMA((18,)),
            pltpu.SemaphoreType.DMA((18,)),
            pltpu.SemaphoreType.DMA((N_MESSAGES * 4,)),
            pltpu.SemaphoreType.DMA((N_MESSAGES * 4,)),
            pltpu.SemaphoreType.DMA((N_MESSAGES * 4,)),
            pltpu.SemaphoreType.DMA((N_MESSAGES * 4,)),
            pltpu.SemaphoreType.DMA,
            pltpu.SemaphoreType.DMA,
        ],
        compiler_params=pltpu.CompilerParams(
            collective_id=0, has_side_effects=True, vmem_limit_bytes=GATHER_LIMIT * 1024 * 1024
        ),
    )(*hbm)
    query, key, value, f_query, f_key, f_value, norm = pl.pallas_call(
        write_kernel,
        out_shape=(
            jax.ShapeDtypeStruct((D_MODEL, COLS), bf16),
            jax.ShapeDtypeStruct((D_MODEL, COLS), bf16),
            jax.ShapeDtypeStruct((D_MODEL, COLS), bf16),
            jax.ShapeDtypeStruct((8, 128), f32),
            jax.ShapeDtypeStruct((8, 128), f32),
            jax.ShapeDtypeStruct((8, 128), f32),
            jax.ShapeDtypeStruct((32, 128), bf16),
        ),
        in_specs=[vmem] * 6,
        out_specs=[any_spec] * 3 + [vmem] * 4,
        scratch_shapes=[
            pltpu.VMEM((16, 3, ROWS, COLS), bf16),
            pltpu.VMEM((8, 3, 64, COLS), bf16),
            pltpu.SemaphoreType.DMA((144,)),
        ],
        compiler_params=pltpu.CompilerParams(vmem_limit_bytes=WRITE_LIMIT * 1024 * 1024),
    )(*state)
    return (
        query, key, value,
        f_query.reshape(COLS), f_key.reshape(COLS), f_value.reshape(COLS), norm.reshape(D_MODEL),
    )


def solution(mesh):
    return jax.shard_map(
        per_device,
        mesh=mesh,
        in_specs=(
            P("zero", "model"), P("zero", None), P(None, "model"),
            P("zero", "model"), P("zero", None), P(None, "model"),
            P("zero", "model"), P("zero", None), P(None, "model"),
            P(("zero", "model")), P(("zero", "model")),
        ),
        out_specs=(
            P(None, "model"), P(None, "model"), P(None, "model"),
            P("model"), P("model"), P("model"), P(),
        ),
        check_vma=False,
    )
```

```python
import jax
import jax.numpy as jnp
from jax import lax
from jax.experimental import pallas as pl
from jax.experimental.pallas import tpu as pltpu
from jax.sharding import PartitionSpec as P

MESH = pl.DeviceIdType.MESH
D_MODEL = 4096
COLS = 1024
ROWS = 128
SUB = 32
SIDE = 4
GATHER_LIMIT = 16
WRITE_LIMIT = 16

MESSAGES = (
    (0, 0, 0, 2),
    (0, 0, 1, 2),
    (-1, 0, 0, 1),
    (0, -1, 1, 2),
    (0, 1, 1, 2),
    (0, 2, 1, 2),
    (-1, 0, 1, 1),
    (-1, -1, 1, 1),
    (-1, 1, 1, 1),
    (-1, 2, 1, 1),
)
N_MESSAGES = len(MESSAGES)


def scaled(low_rows, mixes, inverse, rows, start, source, store):
    low = low_rows[pl.ds(start, rows), :]
    for m in range(3):
        for pair in range(4):
            cols = slice(pair * 256, pair * 256 + 256)
            product = jnp.dot(low, mixes[m, :, cols], preferred_element_type=jnp.float32)
            for j in range(2):
                at = pair * 256 + j * 128
                row = m * 8 + pair * 2 + j
                whole = source[m, pl.ds(start, rows), at : at + 128].astype(jnp.float32) + product[:, j * 128 : j * 128 + 128]
                store(m, at, (whole * inverse[row : row + 1, :]).astype(jnp.bfloat16))


def gather_kernel(
    w_query, w_key, w_value, low_query, low_key, low_value, high_query, high_key, high_value, train, step,
    factors, inverse, norm, low_rows, mixes, full,
    lows, highs, message, from_y, from_core, from_first, from_second,
    load_sem, small_send, small_recv, send_sem, recv_sem, pass_send, pass_recv, own_send, own_recv,
):
    zero, y = lax.axis_index("zero"), lax.axis_index("model")
    z, x, core = zero // 8, zero // 2 % 4, zero % 2
    partner = zero + 1 - 2 * core
    own = pl.multiple_of(zero * ROWS, ROWS)
    first = x + core * (z - x)
    second = z + core * (x - z)

    def index_of(z_at, x_at, core_at):
        return (z_at * 4 + x_at) * 2 + core_at

    def peer(axis, k):
        return index_of((z + axis * k) % 4, (x + (1 - axis) * k) % 4, core)

    def remote(src, dst, sems, at, target, y_at):
        return pltpu.make_async_remote_copy(
            src_ref=src, dst_ref=dst, send_sem=sems[0].at[at], recv_sem=sems[1].at[at],
            device_id=(target, y_at), device_id_type=MESH,
        )

    small = (small_send, small_recv)
    place = second * 4 + first
    loads = [
        pltpu.make_async_copy(src, dst, load_sem.at[k])
        for k, (src, dst) in enumerate(
            (
                (w_query, full.at[0, pl.ds(own, ROWS), :]),
                (w_key, full.at[1, pl.ds(own, ROWS), :]),
                (w_value, full.at[2, pl.ds(own, ROWS), :]),
                (low_query, lows.at[core, place, pl.ds(0, 16), :]),
                (low_key, lows.at[core, place, pl.ds(16, 16), :]),
                (low_value, lows.at[core, place, pl.ds(32, 16), :]),
                (high_query, highs.at[0]), (high_key, highs.at[1]), (high_value, highs.at[2]),
            )
        )
    ]
    for load in loads:
        load.start()

    barrier = pltpu.get_barrier_semaphore()
    pl.semaphore_signal(barrier, inc=1, device_id=(partner, y), device_id_type=MESH)
    for k in range(1, SIDE):
        pl.semaphore_signal(barrier, inc=1, device_id=(peer(0, k), y), device_id_type=MESH)
        pl.semaphore_signal(barrier, inc=1, device_id=(peer(1, k), y), device_id_type=MESH)
        pl.semaphore_signal(barrier, inc=1, device_id=(zero, (y + k) % 4), device_id_type=MESH)

    gain = train[...] + step[...]
    gain = pltpu.roll(jnp.concatenate([gain, jnp.zeros((1, 96), jnp.float32)], axis=1), 32 * y, 1)
    row = lax.broadcasted_iota(jnp.int32, (8, 128), 0)
    tile = jnp.where(row == x * 2 + core, jnp.broadcast_to(gain, (8, 128)), 0.0)
    from_y[pl.ds(y, 1)] = tile[None]
    for load in loads[:3]:
        load.wait()
    pl.semaphore_wait(barrier, 10)

    def rows_of(link, at, arriving, core_at):
        along, across, half, parts = MESSAGES[at]
        axis, way = link // 2, 1 - 2 * (link % 2)
        along = (along - arriving) * way
        z_at = (z + axis * along + (1 - axis) * across + 8) % 4
        x_at = (x + (1 - axis) * along + axis * across + 8) % 4
        half = axis if half == 0 else 1 - axis
        part = link % 2 if parts == 1 else 0
        return pl.multiple_of(index_of(z_at, x_at, core_at) * ROWS + half * 64 + part * SUB, SUB)

    def chunk_of(link, at, arriving, core_at):
        return full.at[:, pl.ds(rows_of(link, at, arriving, core_at), MESSAGES[at][3] * SUB), :]

    def link_copy(link, at, arriving=0):
        axis, way = link // 2, 1 - 2 * (link % 2)
        chunk = chunk_of(link, at, arriving, core)
        target = index_of((z + axis * way + 4) % 4, (x + (1 - axis) * way + 4) % 4, core)
        return remote(chunk, chunk, (send_sem, recv_sem), at * 4 + link, target, y)

    def pass_copy(link, at):
        chunk = chunk_of(link, at, 1, core)
        return remote(chunk, chunk, (pass_send, pass_recv), at * 4 + link, partner, y)

    def each_link(body, count=4):
        def step_of(link, carry):
            body(link)
            return carry

        lax.fori_loop(0, count, step_of, 0)

    def send(at):
        each_link(lambda link: link_copy(link, at).start())

    def arrive(at):
        def body(link):
            link_copy(link, at, 1).wait_recv()
            pass_copy(link, at).start()

        each_link(body)

    send(0)
    block = full.at[:, pl.ds(own, ROWS), :]
    own_copy = pltpu.make_async_remote_copy(
        src_ref=block, dst_ref=block, send_sem=own_send, recv_sem=own_recv,
        device_id=(partner, y), device_id_type=MESH,
    )
    own_copy.start()
    y_copies = [
        remote(from_y.at[y], from_y.at[y], small, k, zero, (y + k) % 4) for k in range(1, SIDE)
    ]
    for copy in y_copies:
        copy.start()

    for load in loads[3:]:
        load.wait()
    low_own = lows.at[core, place]
    low_first = [remote(low_own, low_own, small, 10 + k, peer(core, k), y) for k in range(1, SIDE)]
    for copy in low_first:
        copy.start()
    send(1)
    for m in range(3):
        product = lax.dot_general(
            low_own[16 * m : 16 * m + 16, :], highs[m], (((0,), (0,)), ((), ())),
            preferred_element_type=jnp.float32,
        )
        value = full[m, pl.ds(own, ROWS), :].astype(jnp.float32) + 0.5 * product
        total = jnp.sum(jnp.abs(value), axis=0, keepdims=True)
        for j in range(8):
            message[m * 8 + j : m * 8 + j + 1, :] = total[:, j * 128 : (j + 1) * 128]
        mixes[m] = jnp.zeros((128, COLS), jnp.bfloat16)
        mixes[m, 16 * m : 16 * m + 16, :] = (0.5 * highs[m].astype(jnp.float32)).astype(jnp.bfloat16)
    for copy in y_copies:
        copy.wait()
    message[24:32, :] = from_y[0] + from_y[1] + from_y[2] + from_y[3]

    core_copy = remote(message, from_core, small, 0, partner, y)
    core_copy.start()
    core_copy.wait()
    share = 1 - core
    mine = pl.ds(pl.multiple_of(share * 16, 16), 16)
    from_first[pl.ds(first, 1)] = (message[mine, :] + from_core[mine, :])[None]
    first_copies = [
        remote(from_first.at[first], from_first.at[first], small, 3 + k, peer(core, k), y)
        for k in range(1, SIDE)
    ]
    for copy in first_copies:
        copy.start()

    arrive(0)
    send(2)
    send(3)
    for copy in first_copies + low_first:
        copy.wait()
    from_second[pl.ds(share, 1), pl.ds(second, 1)] = (
        from_first[0] + from_first[1] + from_first[2] + from_first[3]
    )[None, None]
    own_sum = from_second.at[share, second]
    second_copies = [remote(own_sum, own_sum, small, 6 + k, peer(1 - core, k), y) for k in range(1, SIDE)]
    low_line = lows.at[core, pl.ds(pl.multiple_of(second * 4, 4), 4)]
    second_copies += [remote(low_line, low_line, small, 13 + k, peer(1 - core, k), y) for k in range(1, SIDE)]
    for copy in second_copies:
        copy.start()

    arrive(1)
    send(4)
    for copy in second_copies:
        copy.wait()
    last_copies = [
        remote(from_second.at[share], from_second.at[share], small, 10, partner, y),
        remote(lows.at[core], lows.at[core], small, 17, partner, y),
    ]
    for copy in last_copies:
        copy.start()
    for copy in last_copies:
        copy.wait()
    sums = [from_second[h, 0] + from_second[h, 1] + from_second[h, 2] + from_second[h, 3] for h in range(2)]
    factor = jnp.concatenate([sums[0], sums[1][:8]], axis=0) / D_MODEL
    factors[...] = factor
    inverse[...] = 1.0 / factor
    for k in range(SIDE):
        norm[k * 8 : (k + 1) * 8, :] = from_second[1, k, 8:16, :].astype(jnp.bfloat16)

    arrive(2)
    send(5)
    lane = lax.broadcasted_iota(jnp.int32, (48, 128), 1)
    unit = jnp.where(lax.broadcasted_iota(jnp.int32, (48, 128), 0) == lane, 1.0, 0.0).astype(jnp.bfloat16)

    def turn(k, carry):
        core_at, major, minor = k // 16, k // 4 % 4, k % 4
        z_at = major + core_at * (minor - major)
        x_at = minor + core_at * (major - minor)
        start = pl.multiple_of(index_of(z_at, x_at, core_at) * ROWS, ROWS)
        turned = lax.dot_general(
            lows[core_at, k % 16], unit, (((0,), (0,)), ((), ())), preferred_element_type=jnp.float32
        )
        low_rows[pl.ds(start, ROWS), :] = turned.astype(jnp.bfloat16)
        return carry

    lax.fori_loop(0, 32, turn, 0)

    scale = inverse[...]

    def scale_rows(start):
        def store(m, at, value):
            full[m, pl.ds(start, 64), at : at + 128] = value

        scaled(low_rows, mixes, scale, 64, start, full, store)

    def scale_passed(at):
        def body(link):
            pass_copy(link, at).wait_recv()
            scale_rows(pl.multiple_of(rows_of(link, at, 1, 1 - core), 64))

        each_link(body)

    def scale_passed_pair(at):
        def body(axis):
            pass_copy(2 * axis, at).wait_recv()
            pass_copy(2 * axis + 1, at).wait_recv()
            scale_rows(pl.multiple_of(rows_of(2 * axis, at, 1, 1 - core), 64))

        each_link(body, 2)

    def scale_mine(at):
        def body(link):
            pass_copy(link, at).wait_send()
            scale_rows(pl.multiple_of(rows_of(link, at, 1, core), 64))

        each_link(body)

    def scale_mine_pair(at):
        def body(axis):
            pass_copy(2 * axis, at).wait_send()
            pass_copy(2 * axis + 1, at).wait_send()
            scale_rows(pl.multiple_of(rows_of(2 * axis, at, 1, core), 64))

        each_link(body, 2)

    def sent(at):
        each_link(lambda link: link_copy(link, at).wait_send())

    own_copy.wait_recv()
    each_link(lambda half: scale_rows(pl.multiple_of(partner * ROWS + half * 64, 64)), 2)
    scale_passed(0)
    sent(0)
    sent(1)
    own_copy.wait_send()
    each_link(lambda half: scale_rows(pl.multiple_of(zero * ROWS + half * 64, 64)), 2)
    arrive(3)
    send(6)
    send(7)
    scale_passed(1)
    scale_passed_pair(2)
    arrive(4)
    send(8)
    scale_passed(3)
    sent(2)
    sent(3)
    sent(4)
    scale_mine(0)
    arrive(5)
    send(9)
    scale_passed(4)
    sent(5)
    scale_mine_pair(2)
    arrive(6)
    sent(6)
    scale_mine(1)
    scale_passed(5)
    arrive(7)
    sent(7)
    scale_mine(3)
    scale_mine_pair(6)
    scale_passed_pair(6)
    arrive(8)
    sent(8)
    scale_mine(4)
    scale_mine_pair(7)
    scale_passed_pair(7)
    arrive(9)
    sent(9)
    scale_mine(5)
    scale_mine_pair(8)
    scale_passed_pair(8)
    each_link(lambda link: pass_copy(link, 9).wait())


def write_kernel(
    factors, inverse, norm, low_rows, mixes, full,
    query, key, value, f_query, f_key, f_value, norm_out, late, sem,
):
    zero = lax.axis_index("zero")
    z, x = zero // 8, zero // 2 % 4
    outs = (query, key, value)

    def start_of(k):
        return pl.multiple_of(((z + 2 + k // 4) % 4 * 4 + (x + 2 + k % 4) % 4) * 2 * ROWS, 2 * ROWS)

    def ready_copy(k, m):
        rows = pl.ds(start_of(k), 2 * ROWS)
        return pltpu.make_async_copy(full.at[m, rows, :], outs[m].at[rows, :], sem.at[k * 3 + m])

    def late_copy(m):
        return pltpu.make_async_copy(late.at[m], outs[m].at[pl.ds(start_of(0), 2 * ROWS), :], sem.at[m])

    def start_ready(k, carry):
        for m in range(3):
            ready_copy(k, m).start()
        return carry

    def wait_ready(k, carry):
        for m in range(3):
            ready_copy(k, m).wait()
        return carry

    lax.fori_loop(1, 16, start_ready, 0)
    for m, out in enumerate((f_query, f_key, f_value)):
        out[...] = factors[m * 8 : (m + 1) * 8, :]
    norm_out[...] = norm[...]
    scale = inverse[...]

    def scale_late(k, carry):
        def store(m, at, value):
            late[m, pl.ds(pl.multiple_of(k * 64, 64), 64), at : at + 128] = value

        scaled(low_rows, mixes, scale, 64, pl.multiple_of(start_of(0) + k * 64, 64), full, store)
        return carry

    lax.fori_loop(0, 4, scale_late, 0)
    for m in range(3):
        late_copy(m).start()
    lax.fori_loop(1, 16, wait_ready, 0)
    for m in range(3):
        late_copy(m).wait()


def per_device(wq, lq, hq, wk, lk, hk, wv, lv, hv, train, step):
    any_spec = pl.BlockSpec(memory_space=pl.ANY)
    vmem = pl.BlockSpec(memory_space=pltpu.VMEM)
    f32, bf16 = jnp.float32, jnp.bfloat16
    hbm = [
        pltpu.with_memory_space_constraint(a, pltpu.HBM)
        for a in (wq, wk, wv, lq.T, lk.T, lv.T, hq, hk, hv, train.reshape(1, 32), step.reshape(1, 32))
    ]
    state = pl.pallas_call(
        gather_kernel,
        out_shape=(
            jax.ShapeDtypeStruct((24, 128), f32),
            jax.ShapeDtypeStruct((24, 128), f32),
            jax.ShapeDtypeStruct((32, 128), bf16),
            pltpu.VMEM((D_MODEL, 128), bf16),
            pltpu.VMEM((3, 128, COLS), bf16),
            pltpu.VMEM((3, D_MODEL, COLS), bf16),
        ),
        in_specs=[any_spec] * 9 + [vmem] * 2,
        out_specs=(vmem,) * 6,
        scratch_shapes=[
            pltpu.VMEM((2, 16, 48, 128), bf16),
            pltpu.VMEM((3, 16, COLS), bf16),
            pltpu.VMEM((32, 128), f32),
            pltpu.VMEM((4, 8, 128), f32),
            pltpu.VMEM((32, 128), f32),
            pltpu.VMEM((4, 16, 128), f32),
            pltpu.VMEM((2, 4, 16, 128), f32),
            pltpu.SemaphoreType.DMA((9,)),
            pltpu.SemaphoreType.DMA((18,)),
            pltpu.SemaphoreType.DMA((18,)),
            pltpu.SemaphoreType.DMA((N_MESSAGES * 4,)),
            pltpu.SemaphoreType.DMA((N_MESSAGES * 4,)),
            pltpu.SemaphoreType.DMA((N_MESSAGES * 4,)),
            pltpu.SemaphoreType.DMA((N_MESSAGES * 4,)),
            pltpu.SemaphoreType.DMA,
            pltpu.SemaphoreType.DMA,
        ],
        compiler_params=pltpu.CompilerParams(
            collective_id=0, has_side_effects=True, vmem_limit_bytes=GATHER_LIMIT * 1024 * 1024
        ),
    )(*hbm)
    query, key, value, f_query, f_key, f_value, norm = pl.pallas_call(
        write_kernel,
        out_shape=(
            jax.ShapeDtypeStruct((D_MODEL, COLS), bf16),
            jax.ShapeDtypeStruct((D_MODEL, COLS), bf16),
            jax.ShapeDtypeStruct((D_MODEL, COLS), bf16),
            jax.ShapeDtypeStruct((8, 128), f32),
            jax.ShapeDtypeStruct((8, 128), f32),
            jax.ShapeDtypeStruct((8, 128), f32),
            jax.ShapeDtypeStruct((32, 128), bf16),
        ),
        in_specs=[vmem] * 6,
        out_specs=[any_spec] * 3 + [vmem] * 4,
        scratch_shapes=[
            pltpu.VMEM((3, 2 * ROWS, COLS), bf16),
            pltpu.SemaphoreType.DMA((48,)),
        ],
        compiler_params=pltpu.CompilerParams(vmem_limit_bytes=WRITE_LIMIT * 1024 * 1024),
    )(*state)
    return (
        query, key, value,
        f_query.reshape(COLS), f_key.reshape(COLS), f_value.reshape(COLS), norm.reshape(D_MODEL),
    )


def solution(mesh):
    return jax.shard_map(
        per_device,
        mesh=mesh,
        in_specs=(
            P("zero", "model"), P("zero", None), P(None, "model"),
            P("zero", "model"), P("zero", None), P(None, "model"),
            P("zero", "model"), P("zero", None), P(None, "model"),
            P(("zero", "model")), P(("zero", "model")),
        ),
        out_specs=(
            P(None, "model"), P(None, "model"), P(None, "model"),
            P("model"), P("model"), P("model"), P(),
        ),
        check_vma=False,
    )
```

```python
import jax
import jax.numpy as jnp
from jax import lax
from jax.experimental import pallas as pl
from jax.experimental.pallas import tpu as pltpu
from jax.sharding import PartitionSpec as P

MESH = pl.DeviceIdType.MESH
D_MODEL = 4096
COLS = 1024
ROWS = 128
SUB = 32
SIDE = 4
GATHER_LIMIT = 16
WRITE_LIMIT = 16

MESSAGES = (
    (0, 0, 0, 2, 0, 64),
    (0, 0, 1, 2, 0, 64),
    (-1, 0, 0, 1, 0, 32),
    (0, -1, 1, 2, 0, 64),
    (0, 1, 1, 2, 0, 64),
    (0, 2, 1, 2, 0, 64),
    (-1, 0, 1, 1, 0, 32),
    (-1, -1, 1, 1, 0, 32),
    (-1, 1, 1, 1, 0, 32),
    (-1, 2, 1, 1, 0, 32),
)
N_MESSAGES = len(MESSAGES)


def scaled(low_rows, mixes, inverse, rows, start, source, store):
    low = low_rows[pl.ds(start, rows), :]
    for m in range(3):
        for pair in range(4):
            cols = slice(pair * 256, pair * 256 + 256)
            product = jnp.dot(low, mixes[m, :, cols], preferred_element_type=jnp.float32)
            for j in range(2):
                at = pair * 256 + j * 128
                row = m * 8 + pair * 2 + j
                whole = source[m, pl.ds(start, rows), at : at + 128].astype(jnp.float32) + product[:, j * 128 : j * 128 + 128]
                store(m, at, (whole * inverse[row : row + 1, :]).astype(jnp.bfloat16))


def gather_kernel(
    w_query, w_key, w_value, low_query, low_key, low_value, high_query, high_key, high_value, train, step,
    factors, inverse, norm, low_rows, mixes, full,
    gains, low_own, lows, highs, message, from_y, from_core, from_first, from_second,
    load_sem, small_send, small_recv, send_sem, recv_sem, pass_send, pass_recv, own_send, own_recv,
):
    zero, y = lax.axis_index("zero"), lax.axis_index("model")
    z, x, core = zero // 8, zero // 2 % 4, zero % 2
    partner = zero + 1 - 2 * core
    own = pl.multiple_of(zero * ROWS, ROWS)
    first = x + core * (z - x)
    second = z + core * (x - z)

    def index_of(z_at, x_at, core_at):
        return (z_at * 4 + x_at) * 2 + core_at

    def peer(axis, k):
        return index_of((z + axis * k) % 4, (x + (1 - axis) * k) % 4, core)

    def remote(src, dst, sems, at, target, y_at):
        return pltpu.make_async_remote_copy(
            src_ref=src, dst_ref=dst, send_sem=sems[0].at[at], recv_sem=sems[1].at[at],
            device_id=(target, y_at), device_id_type=MESH,
        )

    small = (small_send, small_recv)
    place = second * 4 + first
    loads = [
        pltpu.make_async_copy(src, dst, load_sem.at[k])
        for k, (src, dst) in enumerate(
            (
                (train, gains.at[0]), (step, gains.at[1]),
                (w_query, full.at[0, pl.ds(own, ROWS), :]),
                (w_key, full.at[1, pl.ds(own, ROWS), :]),
                (w_value, full.at[2, pl.ds(own, ROWS), :]),
                (low_query, low_own.at[0]), (low_key, low_own.at[1]), (low_value, low_own.at[2]),
                (high_query, highs.at[0]), (high_key, highs.at[1]), (high_value, highs.at[2]),
            )
        )
    ]
    for load in loads:
        load.start()

    barrier = pltpu.get_barrier_semaphore()
    pl.semaphore_signal(barrier, inc=1, device_id=(partner, y), device_id_type=MESH)
    for k in range(1, SIDE):
        pl.semaphore_signal(barrier, inc=1, device_id=(peer(0, k), y), device_id_type=MESH)
        pl.semaphore_signal(barrier, inc=1, device_id=(peer(1, k), y), device_id_type=MESH)
        pl.semaphore_signal(barrier, inc=1, device_id=(zero, (y + k) % 4), device_id_type=MESH)

    for load in loads[:2]:
        load.wait()
    gain = gains[0] + gains[1]
    gain = pltpu.roll(jnp.concatenate([gain, jnp.zeros((1, 96), jnp.float32)], axis=1), 32 * y, 1)
    row = lax.broadcasted_iota(jnp.int32, (8, 128), 0)
    tile = jnp.where(row == x * 2 + core, jnp.broadcast_to(gain, (8, 128)), 0.0)
    from_y[pl.ds(y, 1)] = tile[None]
    for load in loads[2:5]:
        load.wait()
    pl.semaphore_wait(barrier, 10)

    def rows_of(link, at, arriving, core_at):
        along, across, half, parts, skip, _ = MESSAGES[at]
        axis, way = link // 2, 1 - 2 * (link % 2)
        along = (along - arriving) * way
        z_at = (z + axis * along + (1 - axis) * across + 8) % 4
        x_at = (x + (1 - axis) * along + axis * across + 8) % 4
        half = axis if half == 0 else 1 - axis
        part = link % 2 if parts == 1 else 0
        return pl.multiple_of(index_of(z_at, x_at, core_at) * ROWS + half * 64 + part * SUB + skip, 8)

    def chunk_of(link, at, arriving, core_at):
        return full.at[:, pl.ds(rows_of(link, at, arriving, core_at), MESSAGES[at][5]), :]

    def link_copy(link, at, arriving=0):
        axis, way = link // 2, 1 - 2 * (link % 2)
        chunk = chunk_of(link, at, arriving, core)
        target = index_of((z + axis * way + 4) % 4, (x + (1 - axis) * way + 4) % 4, core)
        return remote(chunk, chunk, (send_sem, recv_sem), at * 4 + link, target, y)

    def pass_copy(link, at):
        chunk = chunk_of(link, at, 1, core)
        return remote(chunk, chunk, (pass_send, pass_recv), at * 4 + link, partner, y)

    def each_link(body, count=4):
        def step_of(link, carry):
            body(link)
            return carry

        lax.fori_loop(0, count, step_of, 0)

    def send(at):
        each_link(lambda link: link_copy(link, at).start())

    def arrive(at):
        def body(link):
            link_copy(link, at, 1).wait_recv()
            pass_copy(link, at).start()

        each_link(body)

    send(0)
    y_copies = [
        remote(from_y.at[y], from_y.at[y], small, k, zero, (y + k) % 4) for k in range(1, SIDE)
    ]
    for copy in y_copies:
        copy.start()

    for load in loads[5:]:
        load.wait()
    lows[core, y, place] = low_own[y - y // 3]
    for m in range(3):
        product = lax.dot_general(
            low_own[m], highs[m], (((0,), (0,)), ((), ())), preferred_element_type=jnp.float32
        )
        value = full[m, pl.ds(own, ROWS), :].astype(jnp.float32) + 0.5 * product
        total = jnp.sum(jnp.abs(value), axis=0, keepdims=True)
        for j in range(8):
            message[m * 8 + j : m * 8 + j + 1, :] = total[:, j * 128 : (j + 1) * 128]
    for copy in y_copies:
        copy.wait()
    message[24:32, :] = from_y[0] + from_y[1] + from_y[2] + from_y[3]

    core_copy = remote(message, from_core, small, 0, partner, y)
    core_copy.start()
    low_block = lows.at[core, y, place]
    low_first = [remote(low_block, low_block, small, 10 + k, peer(core, k), y) for k in range(1, SIDE)]
    for copy in low_first:
        copy.start()
    core_copy.wait()
    share = 1 - core
    mine = pl.ds(pl.multiple_of(share * 16, 16), 16)
    from_first[pl.ds(first, 1)] = (message[mine, :] + from_core[mine, :])[None]
    first_copies = [
        remote(from_first.at[first], from_first.at[first], small, 3 + k, peer(core, k), y)
        for k in range(1, SIDE)
    ]
    for copy in first_copies:
        copy.start()
    send(1)
    block = full.at[:, pl.ds(own, ROWS), :]
    own_copy = pltpu.make_async_remote_copy(
        src_ref=block, dst_ref=block, send_sem=own_send, recv_sem=own_recv,
        device_id=(partner, y), device_id_type=MESH,
    )
    own_copy.start()
    for m in range(3):
        mixes[m] = jnp.zeros((128, COLS), jnp.bfloat16)
        mixes[m, 16 * m : 16 * m + 16, :] = (0.5 * highs[m].astype(jnp.float32)).astype(jnp.bfloat16)

    arrive(0)
    for copy in first_copies + low_first:
        copy.wait()
    from_second[pl.ds(share, 1), pl.ds(second, 1)] = (
        from_first[0] + from_first[1] + from_first[2] + from_first[3]
    )[None, None]
    own_sum = from_second.at[share, second]
    second_copies = [remote(own_sum, own_sum, small, 6 + k, peer(1 - core, k), y) for k in range(1, SIDE)]
    low_line = lows.at[core, y, pl.ds(pl.multiple_of(second * 4, 4), 4)]
    second_copies += [remote(low_line, low_line, small, 13 + k, peer(1 - core, k), y) for k in range(1, SIDE)]
    for copy in second_copies:
        copy.start()
    send(2)
    send(3)

    arrive(1)
    send(4)
    for copy in second_copies:
        copy.wait()
    sum_copy = remote(from_second.at[share], from_second.at[share], small, 10, partner, y)
    sum_copy.start()
    low_plane = lows.at[core, y]
    low_planes = [remote(low_plane, low_plane, small, 17 + k, zero, (y + k) % 4) for k in range(1, SIDE)]
    for copy in low_planes:
        copy.start()
    sum_copy.wait()
    sums = [from_second[h, 0] + from_second[h, 1] + from_second[h, 2] + from_second[h, 3] for h in range(2)]
    factor = jnp.concatenate([sums[0], sums[1][:8]], axis=0) / D_MODEL
    factors[...] = factor
    inverse[...] = 1.0 / factor
    for k in range(SIDE):
        norm[k * 8 : (k + 1) * 8, :] = from_second[1, k, 8:16, :].astype(jnp.bfloat16)

    for copy in low_planes:
        copy.wait()
    low_copy = remote(lows.at[core], lows.at[core], small, 17, partner, y)
    low_copy.start()
    arrive(2)
    send(5)
    low_copy.wait()
    lane = lax.broadcasted_iota(jnp.int32, (48, 128), 1)
    unit = jnp.where(lax.broadcasted_iota(jnp.int32, (48, 128), 0) == lane, 1.0, 0.0).astype(jnp.bfloat16)

    def turn(k, carry):
        core_at, major, minor = k // 16, k // 4 % 4, k % 4
        z_at = major + core_at * (minor - major)
        x_at = minor + core_at * (major - minor)
        start = pl.multiple_of(index_of(z_at, x_at, core_at) * ROWS, ROWS)
        turned = lax.dot_general(
            jnp.concatenate([lows[core_at, m, k % 16] for m in range(3)], axis=0), unit, (((0,), (0,)), ((), ())), preferred_element_type=jnp.float32
        )
        low_rows[pl.ds(start, ROWS), :] = turned.astype(jnp.bfloat16)
        return carry

    lax.fori_loop(0, 32, turn, 0)

    scale = inverse[...]

    def scale_rows(start):
        def store(m, at, value):
            full[m, pl.ds(start, 64), at : at + 128] = value

        scaled(low_rows, mixes, scale, 64, start, full, store)

    def scale_passed(at):
        def body(link):
            pass_copy(link, at).wait_recv()
            scale_rows(pl.multiple_of(rows_of(link, at, 1, 1 - core), 64))

        each_link(body)

    def scale_passed_pair(at):
        def body(axis):
            pass_copy(2 * axis, at).wait_recv()
            pass_copy(2 * axis + 1, at).wait_recv()
            scale_rows(pl.multiple_of(rows_of(2 * axis, at, 1, 1 - core), 64))

        each_link(body, 2)

    def scale_mine(at):
        def body(link):
            pass_copy(link, at).wait_send()
            scale_rows(pl.multiple_of(rows_of(link, at, 1, core), 64))

        each_link(body)

    def scale_mine_pair(at):
        def body(axis):
            pass_copy(2 * axis, at).wait_send()
            pass_copy(2 * axis + 1, at).wait_send()
            scale_rows(pl.multiple_of(rows_of(2 * axis, at, 1, core), 64))

        each_link(body, 2)

    def sent(at):
        each_link(lambda link: link_copy(link, at).wait_send())

    own_copy.wait_recv()
    each_link(lambda half: scale_rows(pl.multiple_of(partner * ROWS + half * 64, 64)), 2)
    scale_passed(0)
    sent(0)
    sent(1)
    own_copy.wait_send()
    each_link(lambda half: scale_rows(pl.multiple_of(zero * ROWS + half * 64, 64)), 2)
    arrive(3)
    send(6)
    send(7)
    scale_passed(1)
    scale_passed_pair(2)
    arrive(4)
    send(8)
    scale_passed(3)
    sent(2)
    sent(3)
    sent(4)
    scale_mine(0)
    arrive(5)
    send(9)
    scale_passed(4)
    sent(5)
    scale_mine_pair(2)
    arrive(6)
    sent(6)
    scale_mine(1)
    scale_passed(5)
    arrive(7)
    sent(7)
    scale_mine(3)
    scale_mine_pair(6)
    scale_passed_pair(6)
    sent(8)
    scale_mine(4)
    arrive(8)
    scale_mine_pair(7)
    scale_passed_pair(7)
    arrive(9)
    sent(9)
    each_link(lambda link: pass_copy(link, 5).wait_send())
    each_link(lambda link: pass_copy(link, 8).wait())
    each_link(lambda link: pass_copy(link, 9).wait())


PARTLY = {
    (2, 2): (),
    (2, 1): ((1, 1),),
    (1, 2): ((0, 1),),
    (3, 2): ((0, 1), (1, 0), (1, 1)),
    (2, 3): ((1, 1), (0, 0), (0, 1)),
}
LATE = 12


def write_kernel(
    factors, inverse, norm, low_rows, mixes, full,
    query, key, value, f_query, f_key, f_value, norm_out, late, sem, late_sem, small_sem,
):
    zero = lax.axis_index("zero")
    z, x, core = zero // 8, zero // 2 % 4, zero % 2
    outs = (query, key, value)

    def start_of(dz, dx, half, other):
        core_at = core + other * (1 - 2 * core)
        return pl.multiple_of((((z + dz) % 4 * 4 + (x + dx) % 4) * 2 + core_at) * ROWS + half * 64, 64)

    runs = []
    for dz in range(4):
        for dx in range(4):
            if (dz, dx) not in PARTLY:
                runs.append((pl.multiple_of(((z + dz) % 4 * 4 + (x + dx) % 4) * 2 * ROWS, 2 * ROWS), 2 * ROWS))
    for (dz, dx), halves in PARTLY.items():
        for half, other in halves:
            runs.append((start_of(dz, dx, half, other), 64))
    copies = []
    for start, rows in runs:
        for m in range(3):
            part = pl.ds(start, rows)
            copies.append(pltpu.make_async_copy(full.at[m, part, :], outs[m].at[part, :], sem.at[len(copies)]))
    copies += [
        pltpu.make_async_copy(src, dst, small_sem.at[k])
        for k, (src, dst) in enumerate(
            (
                (factors.at[pl.ds(0, 8), :], f_query), (factors.at[pl.ds(8, 8), :], f_key),
                (factors.at[pl.ds(16, 8), :], f_value), (norm, norm_out),
            )
        )
    ]
    for copy in copies:
        copy.start()
    scale = inverse[...]

    def late_start(k):
        group, half, turn = k // 4, k // 2 % 2, k % 2
        is_0, is_1, is_2 = (2 - group) * (1 - group) // 2, group * (2 - group), group * (group - 1) // 2
        side = 1 + 2 * turn
        dz = is_0 * 2 + is_1 * (2 - half) + is_2 * ((1 - half) * side + half * 2)
        dx = is_0 * 2 + is_1 * (1 + half) + is_2 * (half * side + (1 - half) * 2)
        return start_of(dz, dx, half, (1 - is_2) * turn)

    def late_copy(k, m):
        return pltpu.make_async_copy(
            late.at[k, m], outs[m].at[pl.ds(late_start(k), 64), :], late_sem.at[k * 3 + m]
        )

    def scale_late(k, carry):
        def store(m, at, value):
            late[k, m, :, at : at + 128] = value

        scaled(low_rows, mixes, scale, 64, late_start(k), full, store)
        for m in range(3):
            late_copy(k, m).start()
        return carry

    def wait_late(k, carry):
        for m in range(3):
            late_copy(k, m).wait()
        return carry

    lax.fori_loop(0, LATE, scale_late, 0)
    for copy in copies:
        copy.wait()
    lax.fori_loop(0, LATE, wait_late, 0)


def per_device(wq, lq, hq, wk, lk, hk, wv, lv, hv, train, step):
    any_spec = pl.BlockSpec(memory_space=pl.ANY)
    vmem = pl.BlockSpec(memory_space=pltpu.VMEM)
    f32, bf16 = jnp.float32, jnp.bfloat16
    hbm = [
        pltpu.with_memory_space_constraint(a, pltpu.HBM)
        for a in (wq, wk, wv, lq.T, lk.T, lv.T, hq, hk, hv, train.reshape(1, 32), step.reshape(1, 32))
    ]
    state = pl.pallas_call(
        gather_kernel,
        out_shape=(
            jax.ShapeDtypeStruct((24, 128), f32),
            jax.ShapeDtypeStruct((24, 128), f32),
            jax.ShapeDtypeStruct((32, 128), bf16),
            pltpu.VMEM((D_MODEL, 128), bf16),
            pltpu.VMEM((3, 128, COLS), bf16),
            pltpu.VMEM((3, D_MODEL, COLS), bf16),
        ),
        in_specs=[any_spec] * 11,
        out_specs=(vmem,) * 6,
        scratch_shapes=[
            pltpu.VMEM((2, 1, 32), f32),
            pltpu.VMEM((3, 16, 128), bf16),
            pltpu.VMEM((2, 4, 16, 16, 128), bf16),
            pltpu.VMEM((3, 16, COLS), bf16),
            pltpu.VMEM((32, 128), f32),
            pltpu.VMEM((4, 8, 128), f32),
            pltpu.VMEM((32, 128), f32),
            pltpu.VMEM((4, 16, 128), f32),
            pltpu.VMEM((2, 4, 16, 128), f32),
            pltpu.SemaphoreType.DMA((11,)),
            pltpu.SemaphoreType.DMA((21,)),
            pltpu.SemaphoreType.DMA((21,)),
            pltpu.SemaphoreType.DMA((N_MESSAGES * 4,)),
            pltpu.SemaphoreType.DMA((N_MESSAGES * 4,)),
            pltpu.SemaphoreType.DMA((N_MESSAGES * 4,)),
            pltpu.SemaphoreType.DMA((N_MESSAGES * 4,)),
            pltpu.SemaphoreType.DMA,
            pltpu.SemaphoreType.DMA,
        ],
        compiler_params=pltpu.CompilerParams(
            collective_id=0, has_side_effects=True, vmem_limit_bytes=GATHER_LIMIT * 1024 * 1024
        ),
    )(*hbm)
    query, key, value, f_query, f_key, f_value, norm = pl.pallas_call(
        write_kernel,
        out_shape=(
            jax.ShapeDtypeStruct((D_MODEL, COLS), bf16),
            jax.ShapeDtypeStruct((D_MODEL, COLS), bf16),
            jax.ShapeDtypeStruct((D_MODEL, COLS), bf16),
            jax.ShapeDtypeStruct((8, 128), f32),
            jax.ShapeDtypeStruct((8, 128), f32),
            jax.ShapeDtypeStruct((8, 128), f32),
            jax.ShapeDtypeStruct((32, 128), bf16),
        ),
        in_specs=[vmem] * 6,
        out_specs=[any_spec] * 7,
        scratch_shapes=[
            pltpu.VMEM((LATE, 3, 64, COLS), bf16),
            pltpu.SemaphoreType.DMA((57,)),
            pltpu.SemaphoreType.DMA((LATE * 3,)),
            pltpu.SemaphoreType.DMA((4,)),
        ],
        compiler_params=pltpu.CompilerParams(vmem_limit_bytes=WRITE_LIMIT * 1024 * 1024),
    )(*state)
    return (
        query, key, value,
        f_query.reshape(COLS), f_key.reshape(COLS), f_value.reshape(COLS), norm.reshape(D_MODEL),
    )


def solution(mesh):
    return jax.shard_map(
        per_device,
        mesh=mesh,
        in_specs=(
            P("zero", "model"), P("zero", None), P(None, "model"),
            P("zero", "model"), P("zero", None), P(None, "model"),
            P("zero", "model"), P("zero", None), P(None, "model"),
            P(("zero", "model")), P(("zero", "model")),
        ),
        out_specs=(
            P(None, "model"), P(None, "model"), P(None, "model"),
            P("model"), P("model"), P("model"), P(),
        ),
        check_vma=False,
    )
```

```python
import jax
import jax.numpy as jnp
from jax import lax
from jax.experimental import pallas as pl
from jax.experimental.pallas import tpu as pltpu
from jax.sharding import PartitionSpec as P

MESH = pl.DeviceIdType.MESH
D_MODEL = 4096
COLS = 1024
ROWS = 128
SUB = 32
SIDE = 4
GATHER_LIMIT = 16
WRITE_LIMIT = 16

MESSAGES = (
    (0, 0, 0, 2, 0, 64),
    (0, 0, 1, 2, 0, 64),
    (-1, 0, 0, 1, 0, 32),
    (0, -1, 1, 2, 0, 64),
    (0, 1, 1, 2, 0, 64),
    (0, 2, 1, 2, 0, 64),
    (-1, 0, 1, 1, 0, 32),
    (-1, -1, 1, 1, 0, 32),
    (-1, 1, 1, 1, 0, 32),
    (-1, 2, 1, 1, 0, 24),
    (-1, 2, 1, 1, 24, 8),
)
N_MESSAGES = len(MESSAGES)


def scaled(low_rows, mixes, inverse, rows, start, source, store):
    low = low_rows[pl.ds(start, rows), :]
    for m in range(3):
        for pair in range(4):
            cols = slice(pair * 256, pair * 256 + 256)
            product = jnp.dot(low, mixes[m, :, cols], preferred_element_type=jnp.float32)
            for j in range(2):
                at = pair * 256 + j * 128
                row = m * 8 + pair * 2 + j
                whole = source[m, pl.ds(start, rows), at : at + 128].astype(jnp.float32) + product[:, j * 128 : j * 128 + 128]
                store(m, at, (whole * inverse[row : row + 1, :]).astype(jnp.bfloat16))


def gather_kernel(
    w_query, w_key, w_value, low_query, low_key, low_value, high_query, high_key, high_value, train, step,
    factors, inverse, norm, low_rows, mixes, full,
    gains, low_own, lows, highs, message, from_y, from_core, from_first, from_second,
    load_sem, small_send, small_recv, send_sem, recv_sem, pass_send, pass_recv, own_send, own_recv, near_sem, down_sem,
):
    zero, y = lax.axis_index("zero"), lax.axis_index("model")
    z, x, core = zero // 8, zero // 2 % 4, zero % 2
    partner = zero + 1 - 2 * core
    own = pl.multiple_of(zero * ROWS, ROWS)
    first = x + core * (z - x)
    second = z + core * (x - z)

    def index_of(z_at, x_at, core_at):
        return (z_at * 4 + x_at) * 2 + core_at

    def peer(axis, k):
        return index_of((z + axis * k) % 4, (x + (1 - axis) * k) % 4, core)

    def remote(src, dst, sems, at, target, y_at):
        return pltpu.make_async_remote_copy(
            src_ref=src, dst_ref=dst, send_sem=sems[0].at[at], recv_sem=sems[1].at[at],
            device_id=(target, y_at), device_id_type=MESH,
        )

    def upstream(at, way):
        return at // 2 if way == 1 else (at + 1) // 2 % 2

    near = [
        ((peer(0, 1), y), upstream(x, 1), 0), ((peer(0, 3), y), upstream(x, -1), 0),
        ((peer(1, 1), y), upstream(z, 1), 1), ((peer(1, 3), y), upstream(z, -1), 1),
        ((zero, (y + 1) % 4), upstream(y, 1), 2), ((zero, (y + 3) % 4), upstream(y, -1), 2),
    ]
    greeted = near + [((partner, y), 1 - core, 0)]
    n_up = sum(up for _, up, _ in greeted)

    def wait_down(group):
        n_down = sum(1 - up for _, up, at in greeted if at == group)
        pl.when(n_down > 0)(lambda: pl.semaphore_wait(down_sem.at[group], n_down))

    barrier = pltpu.get_barrier_semaphore()

    def signal(sem, device):
        pl.semaphore_signal(sem, inc=1, device_id=device, device_id_type=MESH)

    for device, up, _ in greeted:
        pl.when(up == 0)(lambda device=device: signal(barrier, device))

    small = (small_send, small_recv)
    place = second * 4 + first
    loads = [
        pltpu.make_async_copy(src, dst, load_sem.at[k])
        for k, (src, dst) in enumerate(
            (
                (train, gains.at[0]), (step, gains.at[1]),
                (w_query, full.at[0, pl.ds(own, ROWS), :]),
                (w_key, full.at[1, pl.ds(own, ROWS), :]),
                (w_value, full.at[2, pl.ds(own, ROWS), :]),
                (low_query, low_own.at[0]), (low_key, low_own.at[1]), (low_value, low_own.at[2]),
                (high_query, highs.at[0]), (high_key, highs.at[1]), (high_value, highs.at[2]),
            )
        )
    ]
    for load in loads:
        load.start()

    for load in loads[:2]:
        load.wait()
    gain = gains[0] + gains[1]
    gain = pltpu.roll(jnp.concatenate([gain, jnp.zeros((1, 96), jnp.float32)], axis=1), 32 * y, 1)
    row = lax.broadcasted_iota(jnp.int32, (8, 128), 0)
    tile = jnp.where(row == x * 2 + core, jnp.broadcast_to(gain, (8, 128)), 0.0)
    message[24:32, :] = tile
    pl.when(n_up > 0)(lambda: pl.semaphore_wait(barrier, n_up))
    for device, up, group in greeted:
        pl.when(up == 1)(lambda device=device, group=group: signal(down_sem.at[group], device))
    for load in loads[2:5]:
        load.wait()

    def rows_of(link, at, arriving, core_at):
        along, across, half, parts, skip, _ = MESSAGES[at]
        axis, way = link // 2, 1 - 2 * (link % 2)
        along = (along - arriving) * way
        z_at = (z + axis * along + (1 - axis) * across + 8) % 4
        x_at = (x + (1 - axis) * along + axis * across + 8) % 4
        half = axis if half == 0 else 1 - axis
        part = link % 2 if parts == 1 else 0
        return pl.multiple_of(index_of(z_at, x_at, core_at) * ROWS + half * 64 + part * SUB + skip, 8)

    def chunk_of(link, at, arriving, core_at):
        return full.at[:, pl.ds(rows_of(link, at, arriving, core_at), MESSAGES[at][5]), :]

    def link_copy(link, at, arriving=0):
        axis, way = link // 2, 1 - 2 * (link % 2)
        chunk = chunk_of(link, at, arriving, core)
        target = index_of((z + axis * way + 4) % 4, (x + (1 - axis) * way + 4) % 4, core)
        return remote(chunk, chunk, (send_sem, recv_sem), at * 4 + link, target, y)

    def pass_copy(link, at):
        chunk = chunk_of(link, at, 1, core)
        return remote(chunk, chunk, (pass_send, pass_recv), at * 4 + link, partner, y)

    def each_link(body, count=4):
        def step_of(link, carry):
            body(link)
            return carry

        lax.fori_loop(0, count, step_of, 0)

    def send(at):
        each_link(lambda link: link_copy(link, at).start())

    def arrive(at):
        def body(link):
            link_copy(link, at, 1).wait_recv()
            pass_copy(link, at).start()

        each_link(body)

    def send_first(to_up, axes):
        def body(back):
            for axis in axes:
                at = (x, z)[axis]
                up = (1 - back) * (at // 2) + back * ((at + 1) // 2 % 2)
                pl.when(up == to_up)(lambda axis=axis: link_copy(2 * axis + back, 0).start())

        each_link(body, 2)

    send_first(1, (0, 1))
    wait_down(0)
    send_first(0, (0,))

    for load in loads[5:]:
        load.wait()
    lows[core, y, place] = low_own[y - y // 3]
    for m in range(3):
        product = lax.dot_general(
            low_own[m], highs[m], (((0,), (0,)), ((), ())), preferred_element_type=jnp.float32
        )
        value = full[m, pl.ds(own, ROWS), :].astype(jnp.float32) + 0.5 * product
        total = jnp.sum(jnp.abs(value), axis=0, keepdims=True)
        for j in range(8):
            message[m * 8 + j : m * 8 + j + 1, :] = total[:, j * 128 : (j + 1) * 128]

    core_copy = remote(message, from_core, small, 0, partner, y)
    core_copy.start()
    wait_down(1)
    send_first(0, (1,))
    wait_down(2)
    for device, _, _ in near:
        signal(near_sem, device)
    pl.semaphore_wait(near_sem, 6)
    low_block = lows.at[core, y, place]
    low_first = [remote(low_block, low_block, small, 10 + k, peer(core, k), y) for k in range(1, SIDE)]
    for copy in low_first:
        copy.start()
    core_copy.wait()
    share = 1 - core
    mine = pl.ds(pl.multiple_of(share * 16, 16), 16)
    from_first[pl.ds(first, 1)] = (message[mine, :] + from_core[mine, :])[None]
    first_copies = [
        remote(from_first.at[first], from_first.at[first], small, 3 + k, peer(core, k), y)
        for k in range(1, SIDE)
    ]
    for copy in first_copies:
        copy.start()
    send(1)
    block = full.at[:, pl.ds(own, ROWS), :]
    own_copy = pltpu.make_async_remote_copy(
        src_ref=block, dst_ref=block, send_sem=own_send, recv_sem=own_recv,
        device_id=(partner, y), device_id_type=MESH,
    )
    own_copy.start()
    for m in range(3):
        mixes[m] = jnp.zeros((128, COLS), jnp.bfloat16)
        mixes[m, 16 * m : 16 * m + 16, :] = (0.5 * highs[m].astype(jnp.float32)).astype(jnp.bfloat16)

    arrive(0)
    for copy in first_copies + low_first:
        copy.wait()
    from_second[pl.ds(share, 1), pl.ds(second, 1)] = (
        from_first[0] + from_first[1] + from_first[2] + from_first[3]
    )[None, None]
    own_sum = from_second.at[share, second]
    second_copies = [remote(own_sum, own_sum, small, 6 + k, peer(1 - core, k), y) for k in range(1, SIDE)]
    low_line = lows.at[core, y, pl.ds(pl.multiple_of(second * 4, 4), 4)]
    second_copies += [remote(low_line, low_line, small, 13 + k, peer(1 - core, k), y) for k in range(1, SIDE)]
    for copy in second_copies:
        copy.start()
    send(2)
    send(3)

    arrive(1)
    send(4)
    for copy in second_copies:
        copy.wait()
    sum_copy = remote(from_second.at[share], from_second.at[share], small, 10, partner, y)
    sum_copy.start()
    low_plane = lows.at[core, y]
    low_planes = [remote(low_plane, low_plane, small, 17 + k, zero, (y + k) % 4) for k in range(1, SIDE)]
    for copy in low_planes:
        copy.start()
    sum_copy.wait()
    from_y[pl.ds(y, 1)] = from_second[1, :, 8:16, :][None]
    y_copies = [remote(from_y.at[y], from_y.at[y], small, k, zero, (y + k) % 4) for k in range(1, SIDE)]
    for copy in y_copies:
        copy.start()
    sums = [from_second[h, 0] + from_second[h, 1] + from_second[h, 2] + from_second[h, 3] for h in range(2)]
    factor = jnp.concatenate([sums[0], sums[1][:8]], axis=0) / D_MODEL
    factors[...] = factor
    inverse[...] = 1.0 / factor
    for copy in y_copies:
        copy.wait()
    for k in range(SIDE):
        rows = from_y[0, k] + from_y[1, k] + from_y[2, k] + from_y[3, k]
        norm[k * 8 : (k + 1) * 8, :] = rows.astype(jnp.bfloat16)

    for copy in low_planes:
        copy.wait()
    low_copy = remote(lows.at[core], lows.at[core], small, 17, partner, y)
    low_copy.start()
    arrive(2)
    send(5)
    low_copy.wait()
    lane = lax.broadcasted_iota(jnp.int32, (48, 128), 1)
    unit = jnp.where(lax.broadcasted_iota(jnp.int32, (48, 128), 0) == lane, 1.0, 0.0).astype(jnp.bfloat16)

    def turn(k, carry):
        core_at, major, minor = k // 16, k // 4 % 4, k % 4
        z_at = major + core_at * (minor - major)
        x_at = minor + core_at * (major - minor)
        start = pl.multiple_of(index_of(z_at, x_at, core_at) * ROWS, ROWS)
        turned = lax.dot_general(
            jnp.concatenate([lows[core_at, m, k % 16] for m in range(3)], axis=0), unit, (((0,), (0,)), ((), ())), preferred_element_type=jnp.float32
        )
        low_rows[pl.ds(start, ROWS), :] = turned.astype(jnp.bfloat16)
        return carry

    lax.fori_loop(0, 32, turn, 0)

    scale = inverse[...]

    def scale_rows(start):
        def store(m, at, value):
            full[m, pl.ds(start, 64), at : at + 128] = value

        scaled(low_rows, mixes, scale, 64, start, full, store)

    def scale_passed(at):
        def body(link):
            pass_copy(link, at).wait_recv()
            scale_rows(pl.multiple_of(rows_of(link, at, 1, 1 - core), 64))

        each_link(body)

    def scale_passed_pair(at):
        def body(axis):
            pass_copy(2 * axis, at).wait_recv()
            pass_copy(2 * axis + 1, at).wait_recv()
            scale_rows(pl.multiple_of(rows_of(2 * axis, at, 1, 1 - core), 64))

        each_link(body, 2)

    def scale_mine(at):
        def body(link):
            pass_copy(link, at).wait_send()
            scale_rows(pl.multiple_of(rows_of(link, at, 1, core), 64))

        each_link(body)

    def scale_mine_pair(at):
        def body(axis):
            pass_copy(2 * axis, at).wait_send()
            pass_copy(2 * axis + 1, at).wait_send()
            scale_rows(pl.multiple_of(rows_of(2 * axis, at, 1, core), 64))

        each_link(body, 2)

    def sent(at):
        each_link(lambda link: link_copy(link, at).wait_send())

    own_copy.wait_recv()
    each_link(lambda half: scale_rows(pl.multiple_of(partner * ROWS + half * 64, 64)), 2)
    scale_passed(0)
    sent(0)
    sent(1)
    own_copy.wait_send()
    each_link(lambda half: scale_rows(pl.multiple_of(zero * ROWS + half * 64, 64)), 2)
    arrive(3)
    send(6)
    send(7)
    scale_passed(1)
    scale_passed_pair(2)
    arrive(4)
    send(8)
    scale_passed(3)
    sent(2)
    sent(3)
    sent(4)
    scale_mine(0)
    arrive(5)
    send(9)
    send(10)
    scale_passed(4)
    sent(5)
    scale_mine_pair(2)
    arrive(6)
    sent(6)
    scale_mine(1)
    scale_passed(5)
    arrive(7)
    sent(7)
    scale_mine(3)
    scale_mine_pair(6)
    scale_passed_pair(6)
    sent(8)
    scale_mine(4)
    arrive(8)
    scale_mine_pair(7)
    scale_passed_pair(7)
    arrive(9)
    arrive(10)
    sent(9)
    sent(10)
    each_link(lambda link: pass_copy(link, 5).wait_send())
    each_link(lambda link: pass_copy(link, 8).wait())
    each_link(lambda link: pass_copy(link, 9).wait())
    each_link(lambda link: pass_copy(link, 10).wait())


PARTLY = {
    (2, 2): (),
    (2, 1): ((1, 1),),
    (1, 2): ((0, 1),),
    (3, 2): ((0, 1), (1, 0), (1, 1)),
    (2, 3): ((1, 1), (0, 0), (0, 1)),
}
LATE = 12


def write_kernel(
    factors, inverse, norm, low_rows, mixes, full,
    query, key, value, f_query, f_key, f_value, norm_out, late, sem, late_sem, small_sem,
):
    zero = lax.axis_index("zero")
    z, x, core = zero // 8, zero // 2 % 4, zero % 2
    outs = (query, key, value)

    def start_of(dz, dx, half, other):
        core_at = core + other * (1 - 2 * core)
        return pl.multiple_of((((z + dz) % 4 * 4 + (x + dx) % 4) * 2 + core_at) * ROWS + half * 64, 64)

    runs = []
    for dz in range(4):
        for dx in range(4):
            if (dz, dx) not in PARTLY:
                runs.append((pl.multiple_of(((z + dz) % 4 * 4 + (x + dx) % 4) * 2 * ROWS, 2 * ROWS), 2 * ROWS))
    for (dz, dx), halves in PARTLY.items():
        for half, other in halves:
            runs.append((start_of(dz, dx, half, other), 64))
    copies = []
    for start, rows in runs:
        for m in range(3):
            part = pl.ds(start, rows)
            copies.append(pltpu.make_async_copy(full.at[m, part, :], outs[m].at[part, :], sem.at[len(copies)]))
    copies += [
        pltpu.make_async_copy(src, dst, small_sem.at[k])
        for k, (src, dst) in enumerate(
            (
                (factors.at[pl.ds(0, 8), :], f_query), (factors.at[pl.ds(8, 8), :], f_key),
                (factors.at[pl.ds(16, 8), :], f_value), (norm, norm_out),
            )
        )
    ]
    for copy in copies:
        copy.start()
    scale = inverse[...]

    def late_start(k):
        group, half, turn = k // 4, k // 2 % 2, k % 2
        is_0, is_1, is_2 = (2 - group) * (1 - group) // 2, group * (2 - group), group * (group - 1) // 2
        side = 1 + 2 * turn
        dz = is_0 * 2 + is_1 * (2 - half) + is_2 * ((1 - half) * side + half * 2)
        dx = is_0 * 2 + is_1 * (1 + half) + is_2 * (half * side + (1 - half) * 2)
        return start_of(dz, dx, half, (1 - is_2) * turn)

    def late_copy(k, m):
        return pltpu.make_async_copy(
            late.at[k, m], outs[m].at[pl.ds(late_start(k), 64), :], late_sem.at[k * 3 + m]
        )

    def scale_late(k, carry):
        def store(m, at, value):
            late[k, m, :, at : at + 128] = value

        scaled(low_rows, mixes, scale, 64, late_start(k), full, store)
        for m in range(3):
            late_copy(k, m).start()
        return carry

    def wait_late(k, carry):
        for m in range(3):
            late_copy(k, m).wait()
        return carry

    lax.fori_loop(0, LATE, scale_late, 0)
    for copy in copies:
        copy.wait()
    lax.fori_loop(0, LATE, wait_late, 0)


def per_device(wq, lq, hq, wk, lk, hk, wv, lv, hv, train, step):
    any_spec = pl.BlockSpec(memory_space=pl.ANY)
    vmem = pl.BlockSpec(memory_space=pltpu.VMEM)
    f32, bf16 = jnp.float32, jnp.bfloat16
    hbm = [
        pltpu.with_memory_space_constraint(a, pltpu.HBM)
        for a in (wq, wk, wv, lq.T, lk.T, lv.T, hq, hk, hv, train.reshape(1, 32), step.reshape(1, 32))
    ]
    state = pl.pallas_call(
        gather_kernel,
        out_shape=(
            jax.ShapeDtypeStruct((24, 128), f32),
            jax.ShapeDtypeStruct((24, 128), f32),
            jax.ShapeDtypeStruct((32, 128), bf16),
            pltpu.VMEM((D_MODEL, 128), bf16),
            pltpu.VMEM((3, 128, COLS), bf16),
            pltpu.VMEM((3, D_MODEL, COLS), bf16),
        ),
        in_specs=[any_spec] * 11,
        out_specs=(vmem,) * 6,
        scratch_shapes=[
            pltpu.VMEM((2, 1, 32), f32),
            pltpu.VMEM((3, 16, 128), bf16),
            pltpu.VMEM((2, 4, 16, 16, 128), bf16),
            pltpu.VMEM((3, 16, COLS), bf16),
            pltpu.VMEM((32, 128), f32),
            pltpu.VMEM((4, 4, 8, 128), f32),
            pltpu.VMEM((32, 128), f32),
            pltpu.VMEM((4, 16, 128), f32),
            pltpu.VMEM((2, 4, 16, 128), f32),
            pltpu.SemaphoreType.DMA((11,)),
            pltpu.SemaphoreType.DMA((21,)),
            pltpu.SemaphoreType.DMA((21,)),
            pltpu.SemaphoreType.DMA((N_MESSAGES * 4,)),
            pltpu.SemaphoreType.DMA((N_MESSAGES * 4,)),
            pltpu.SemaphoreType.DMA((N_MESSAGES * 4,)),
            pltpu.SemaphoreType.DMA((N_MESSAGES * 4,)),
            pltpu.SemaphoreType.DMA,
            pltpu.SemaphoreType.DMA,
            pltpu.SemaphoreType.REGULAR,
            pltpu.SemaphoreType.REGULAR((3,)),
        ],
        compiler_params=pltpu.CompilerParams(
            collective_id=0, has_side_effects=True, vmem_limit_bytes=GATHER_LIMIT * 1024 * 1024
        ),
    )(*hbm)
    query, key, value, f_query, f_key, f_value, norm = pl.pallas_call(
        write_kernel,
        out_shape=(
            jax.ShapeDtypeStruct((D_MODEL, COLS), bf16),
            jax.ShapeDtypeStruct((D_MODEL, COLS), bf16),
            jax.ShapeDtypeStruct((D_MODEL, COLS), bf16),
            jax.ShapeDtypeStruct((8, 128), f32),
            jax.ShapeDtypeStruct((8, 128), f32),
            jax.ShapeDtypeStruct((8, 128), f32),
            jax.ShapeDtypeStruct((32, 128), bf16),
        ),
        in_specs=[vmem] * 6,
        out_specs=[any_spec] * 7,
        scratch_shapes=[
            pltpu.VMEM((LATE, 3, 64, COLS), bf16),
            pltpu.SemaphoreType.DMA((57,)),
            pltpu.SemaphoreType.DMA((LATE * 3,)),
            pltpu.SemaphoreType.DMA((4,)),
        ],
        compiler_params=pltpu.CompilerParams(vmem_limit_bytes=WRITE_LIMIT * 1024 * 1024),
    )(*state)
    return (
        query, key, value,
        f_query.reshape(COLS), f_key.reshape(COLS), f_value.reshape(COLS), norm.reshape(D_MODEL),
    )


def solution(mesh):
    return jax.shard_map(
        per_device,
        mesh=mesh,
        in_specs=(
            P("zero", "model"), P("zero", None), P(None, "model"),
            P("zero", "model"), P("zero", None), P(None, "model"),
            P("zero", "model"), P("zero", None), P(None, "model"),
            P(("zero", "model")), P(("zero", "model")),
        ),
        out_specs=(
            P(None, "model"), P(None, "model"), P(None, "model"),
            P("model"), P("model"), P("model"), P(),
        ),
        check_vma=False,
    )
```

```python
import jax
import jax.numpy as jnp
from jax import lax
from jax.experimental import pallas as pl
from jax.experimental.pallas import tpu as pltpu
from jax.sharding import PartitionSpec as P

MESH = pl.DeviceIdType.MESH
D_MODEL = 4096
COLS = 1024
ROWS = 128
SUB = 32
BLOCK = 64
SIDE = 4
GATHER_LIMIT = 16
WRITE_LIMIT = 16

MESSAGES = (
    (0, 0, 0, 2, 0, 64),
    (0, 0, 1, 2, 0, 64),
    (-1, 0, 0, 1, 0, 32),
    (0, -1, 1, 2, 0, 64),
    (0, 1, 1, 2, 0, 64),
    (0, 2, 1, 2, 0, 64),
    (-1, 0, 1, 1, 0, 32),
    (-1, -1, 1, 1, 0, 32),
    (-1, 1, 1, 1, 0, 32),
    (-1, 2, 1, 1, 0, 24),
    (-1, 2, 1, 1, 24, 8),
)
N_MESSAGES = len(MESSAGES)


def scaled(low_rows, mixes, inverse, rows, start, source, store):
    low = low_rows[pl.ds(start, rows), :]
    for m in range(3):
        for pair in range(4):
            cols = slice(pair * 256, pair * 256 + 256)
            product = jnp.dot(low, mixes[m, :, cols], preferred_element_type=jnp.float32)
            for j in range(2):
                at = pair * 256 + j * 128
                row = m * 8 + pair * 2 + j
                whole = source[m, pl.ds(start, rows), at : at + 128].astype(jnp.float32) + product[:, j * 128 : j * 128 + 128]
                store(m, at, (whole * inverse[row : row + 1, :]).astype(jnp.bfloat16))


def gather_kernel(
    w_query, w_key, w_value, low_query, low_key, low_value, high_query, high_key, high_value, train, step,
    factors, inverse, norm, low_rows, mixes, full,
    gains, low_own, lows, highs, message, from_y, from_core, from_first, from_second,
    load_sem, small_send, small_recv, send_sem, recv_sem, pass_send, pass_recv, own_send, own_recv, near_sem, down_sem,
):
    zero, y = lax.axis_index("zero"), lax.axis_index("model")
    z, x, core = zero // 8, zero // 2 % 4, zero % 2
    partner = zero + 1 - 2 * core
    own = pl.multiple_of(zero * ROWS, ROWS)
    first = x + core * (z - x)
    second = z + core * (x - z)

    def index_of(z_at, x_at, core_at):
        return (z_at * 4 + x_at) * 2 + core_at

    def peer(axis, k):
        return index_of((z + axis * k) % 4, (x + (1 - axis) * k) % 4, core)

    def remote(src, dst, sems, at, target, y_at):
        return pltpu.make_async_remote_copy(
            src_ref=src, dst_ref=dst, send_sem=sems[0].at[at], recv_sem=sems[1].at[at],
            device_id=(target, y_at), device_id_type=MESH,
        )

    def upstream(at, way):
        return at // 2 if way == 1 else (at + 1) // 2 % 2

    near = [
        ((peer(0, 1), y), upstream(x, 1), 0), ((peer(0, 3), y), upstream(x, -1), 0),
        ((peer(1, 1), y), upstream(z, 1), 1), ((peer(1, 3), y), upstream(z, -1), 1),
        ((zero, (y + 1) % 4), upstream(y, 1), 2), ((zero, (y + 3) % 4), upstream(y, -1), 2),
    ]
    greeted = near + [((partner, y), 1 - core, 0)]
    n_up = sum(up for _, up, _ in greeted)

    def wait_down(group):
        n_down = sum(1 - up for _, up, at in greeted if at == group)
        pl.when(n_down > 0)(lambda: pl.semaphore_wait(down_sem.at[group], n_down))

    barrier = pltpu.get_barrier_semaphore()

    def signal(sem, device):
        pl.semaphore_signal(sem, inc=1, device_id=device, device_id_type=MESH)

    for device, up, _ in greeted:
        pl.when(up == 0)(lambda device=device: signal(barrier, device))

    small = (small_send, small_recv)
    place = second * 4 + first
    loads = [
        pltpu.make_async_copy(src, dst, load_sem.at[k])
        for k, (src, dst) in enumerate(
            (
                (w_query, full.at[0, pl.ds(own, ROWS), :]),
                (w_key, full.at[1, pl.ds(own, ROWS), :]),
                (w_value, full.at[2, pl.ds(own, ROWS), :]),
                (low_query, low_own.at[0]), (low_key, low_own.at[1]), (low_value, low_own.at[2]),
                (train, gains.at[0]), (step, gains.at[1]),
                (high_query, highs.at[0]), (high_key, highs.at[1]), (high_value, highs.at[2]),
            )
        )
    ]
    for load in loads[:3]:
        load.start()

    pl.when(n_up > 0)(lambda: pl.semaphore_wait(barrier, n_up))
    for device, up, group in greeted:
        pl.when(up == 1)(lambda device=device, group=group: signal(down_sem.at[group], device))
    for load in loads[3:]:
        load.start()
    for load in loads[:3]:
        load.wait()

    def rows_of(link, at, arriving, core_at):
        along, across, half, parts, skip, _ = MESSAGES[at]
        axis, way = link // 2, 1 - 2 * (link % 2)
        along = (along - arriving) * way
        z_at = (z + axis * along + (1 - axis) * across + 8) % 4
        x_at = (x + (1 - axis) * along + axis * across + 8) % 4
        half = axis if half == 0 else 1 - axis
        part = link % 2 if parts == 1 else 0
        return pl.multiple_of(index_of(z_at, x_at, core_at) * ROWS + half * 64 + part * SUB + skip, 8)

    def chunk_of(link, at, arriving, core_at):
        return full.at[:, pl.ds(rows_of(link, at, arriving, core_at), MESSAGES[at][5]), :]

    def link_copy(link, at, arriving=0):
        axis, way = link // 2, 1 - 2 * (link % 2)
        chunk = chunk_of(link, at, arriving, core)
        target = index_of((z + axis * way + 4) % 4, (x + (1 - axis) * way + 4) % 4, core)
        return remote(chunk, chunk, (send_sem, recv_sem), at * 4 + link, target, y)

    def pass_copy(link, at):
        chunk = chunk_of(link, at, 1, core)
        return remote(chunk, chunk, (pass_send, pass_recv), at * 4 + link, partner, y)

    def each_link(body, count=4):
        def step_of(link, carry):
            body(link)
            return carry

        lax.fori_loop(0, count, step_of, 0)

    def send(at):
        each_link(lambda link: link_copy(link, at).start())

    def arrive(at):
        def body(link):
            link_copy(link, at, 1).wait_recv()
            pass_copy(link, at).start()

        each_link(body)

    def send_first(to_up, axes):
        def body(back):
            for axis in axes:
                at = (x, z)[axis]
                up = (1 - back) * (at // 2) + back * ((at + 1) // 2 % 2)
                pl.when(up == to_up)(lambda axis=axis: link_copy(2 * axis + back, 0).start())

        each_link(body, 2)

    send_first(1, (0, 1))
    wait_down(0)
    send_first(0, (0,))

    for load in loads[6:8]:
        load.wait()
    gain = gains[0] + gains[1]
    gain = pltpu.roll(jnp.concatenate([gain, jnp.zeros((1, 96), jnp.float32)], axis=1), 32 * y, 1)
    row = lax.broadcasted_iota(jnp.int32, (8, 128), 0)
    tile = jnp.where(row == x * 2 + core, jnp.broadcast_to(gain, (8, 128)), 0.0)
    message[24:32, :] = tile

    for load in loads[3:6] + loads[8:]:
        load.wait()
    lows[core, y, place] = low_own[y - y // 3]
    for m in range(3):
        product = lax.dot_general(
            low_own[m], highs[m], (((0,), (0,)), ((), ())), preferred_element_type=jnp.float32
        )
        value = full[m, pl.ds(own, ROWS), :].astype(jnp.float32) + 0.5 * product
        total = jnp.sum(jnp.abs(value), axis=0, keepdims=True)
        for j in range(8):
            message[m * 8 + j : m * 8 + j + 1, :] = total[:, j * 128 : (j + 1) * 128]

    core_copy = remote(message, from_core, small, 0, partner, y)
    core_copy.start()
    wait_down(1)
    send_first(0, (1,))
    wait_down(2)
    for device, _, _ in near:
        signal(near_sem, device)
    pl.semaphore_wait(near_sem, 6)
    low_block = lows.at[core, y, place]
    low_first = [remote(low_block, low_block, small, 10 + k, peer(core, k), y) for k in range(1, SIDE)]
    for copy in low_first:
        copy.start()
    core_copy.wait()
    share = 1 - core
    mine = pl.ds(pl.multiple_of(share * 16, 16), 16)
    from_first[pl.ds(first, 1)] = (message[mine, :] + from_core[mine, :])[None]
    first_copies = [
        remote(from_first.at[first], from_first.at[first], small, 3 + k, peer(core, k), y)
        for k in range(1, SIDE)
    ]
    for copy in first_copies:
        copy.start()
    send(1)
    block = full.at[:, pl.ds(own, ROWS), :]
    own_copy = pltpu.make_async_remote_copy(
        src_ref=block, dst_ref=block, send_sem=own_send, recv_sem=own_recv,
        device_id=(partner, y), device_id_type=MESH,
    )
    own_copy.start()
    for m in range(3):
        mixes[m] = jnp.zeros((128, COLS), jnp.bfloat16)
        mixes[m, 16 * m : 16 * m + 16, :] = (0.5 * highs[m].astype(jnp.float32)).astype(jnp.bfloat16)

    arrive(0)
    for copy in first_copies + low_first:
        copy.wait()
    from_second[pl.ds(share, 1), pl.ds(second, 1)] = (
        from_first[0] + from_first[1] + from_first[2] + from_first[3]
    )[None, None]
    own_sum = from_second.at[share, second]
    second_copies = [remote(own_sum, own_sum, small, 6 + k, peer(1 - core, k), y) for k in range(1, SIDE)]
    low_line = lows.at[core, y, pl.ds(pl.multiple_of(second * 4, 4), 4)]
    second_copies += [remote(low_line, low_line, small, 13 + k, peer(1 - core, k), y) for k in range(1, SIDE)]
    for copy in second_copies:
        copy.start()
    send(2)
    send(3)

    arrive(1)
    send(4)
    for copy in second_copies:
        copy.wait()
    sum_copy = remote(from_second.at[share], from_second.at[share], small, 10, partner, y)
    sum_copy.start()
    low_plane = lows.at[core, y]
    low_planes = [remote(low_plane, low_plane, small, 17 + k, zero, (y + k) % 4) for k in range(1, SIDE)]
    for copy in low_planes:
        copy.start()
    sum_copy.wait()
    from_y[pl.ds(y, 1)] = from_second[1, :, 8:16, :][None]
    y_copies = [remote(from_y.at[y], from_y.at[y], small, k, zero, (y + k) % 4) for k in range(1, SIDE)]
    for copy in y_copies:
        copy.start()
    sums = [from_second[h, 0] + from_second[h, 1] + from_second[h, 2] + from_second[h, 3] for h in range(2)]
    factor = jnp.concatenate([sums[0], sums[1][:8]], axis=0) / D_MODEL
    factors[...] = factor
    inverse[...] = 1.0 / factor
    for copy in y_copies:
        copy.wait()
    for k in range(SIDE):
        rows = from_y[0, k] + from_y[1, k] + from_y[2, k] + from_y[3, k]
        norm[k * 8 : (k + 1) * 8, :] = rows.astype(jnp.bfloat16)

    for copy in low_planes:
        copy.wait()
    low_copy = remote(lows.at[core], lows.at[core], small, 17, partner, y)
    low_copy.start()
    arrive(2)
    send(5)
    low_copy.wait()
    lane = lax.broadcasted_iota(jnp.int32, (48, 128), 1)
    unit = jnp.where(lax.broadcasted_iota(jnp.int32, (48, 128), 0) == lane, 1.0, 0.0).astype(jnp.bfloat16)

    def turn(k, carry):
        core_at, major, minor = k // 16, k // 4 % 4, k % 4
        z_at = major + core_at * (minor - major)
        x_at = minor + core_at * (major - minor)
        start = pl.multiple_of(index_of(z_at, x_at, core_at) * ROWS, ROWS)
        turned = lax.dot_general(
            jnp.concatenate([lows[core_at, m, k % 16] for m in range(3)], axis=0), unit, (((0,), (0,)), ((), ())), preferred_element_type=jnp.float32
        )
        low_rows[pl.ds(start, ROWS), :] = turned.astype(jnp.bfloat16)
        return carry

    lax.fori_loop(0, 32, turn, 0)

    scale = inverse[...]

    def scale_rows(start):
        def store(m, at, value):
            full[m, pl.ds(start, 64), at : at + 128] = value

        scaled(low_rows, mixes, scale, 64, start, full, store)

    def scale_passed(at):
        def body(link):
            pass_copy(link, at).wait_recv()
            scale_rows(pl.multiple_of(rows_of(link, at, 1, 1 - core), 64))

        each_link(body)

    def scale_passed_pair(at):
        def body(axis):
            pass_copy(2 * axis, at).wait_recv()
            pass_copy(2 * axis + 1, at).wait_recv()
            scale_rows(pl.multiple_of(rows_of(2 * axis, at, 1, 1 - core), 64))

        each_link(body, 2)

    def scale_mine(at):
        def body(link):
            pass_copy(link, at).wait_send()
            scale_rows(pl.multiple_of(rows_of(link, at, 1, core), 64))

        each_link(body)

    def scale_mine_pair(at):
        def body(axis):
            pass_copy(2 * axis, at).wait_send()
            pass_copy(2 * axis + 1, at).wait_send()
            scale_rows(pl.multiple_of(rows_of(2 * axis, at, 1, core), 64))

        each_link(body, 2)

    def sent(at):
        each_link(lambda link: link_copy(link, at).wait_send())

    own_copy.wait_recv()
    each_link(lambda half: scale_rows(pl.multiple_of(partner * ROWS + half * 64, 64)), 2)
    scale_passed(0)
    sent(0)
    sent(1)
    own_copy.wait_send()
    each_link(lambda half: scale_rows(pl.multiple_of(zero * ROWS + half * 64, 64)), 2)
    arrive(3)
    send(6)
    send(7)
    scale_passed(1)
    scale_passed_pair(2)
    arrive(4)
    send(8)
    scale_passed(3)
    sent(2)
    sent(3)
    sent(4)
    scale_mine(0)
    arrive(5)
    send(9)
    send(10)
    scale_passed(4)
    sent(5)
    scale_mine_pair(2)
    arrive(6)
    sent(6)
    scale_mine(1)
    arrive(7)
    sent(7)
    scale_mine(3)
    scale_mine_pair(6)
    scale_passed_pair(6)
    sent(8)
    scale_mine(4)
    arrive(8)
    arrive(9)
    arrive(10)
    sent(9)
    sent(10)
    for at in (5, 7, 8):
        each_link(lambda link: pass_copy(link, at).wait())
    each_link(lambda link: pass_copy(link, 9).wait())
    each_link(lambda link: pass_copy(link, 10).wait())


LATE = ((2, 1), (1, 2), (3, 2), (2, 3), (2, 2))


def write_kernel(
    factors, inverse, norm, low_rows, mixes, full,
    query, key, value, f_query, f_key, f_value, norm_out, late, sem, late_sem, small_sem,
):
    zero = lax.axis_index("zero")
    z, x = zero // 8, zero // 2 % 4
    outs = (query, key, value)

    def start_of(dz, dx):
        return pl.multiple_of(((z + dz) % 4 * 4 + (x + dx) % 4) * 2 * ROWS, 2 * ROWS)

    copies = []
    for dz in range(4):
        for dx in range(4):
            if (dz, dx) not in LATE:
                for m in range(3):
                    part = pl.ds(start_of(dz, dx), 2 * ROWS)
                    copies.append(
                        pltpu.make_async_copy(full.at[m, part, :], outs[m].at[part, :], sem.at[len(copies)])
                    )
    copies += [
        pltpu.make_async_copy(src, dst, small_sem.at[k])
        for k, (src, dst) in enumerate(
            (
                (factors.at[pl.ds(0, 8), :], f_query), (factors.at[pl.ds(8, 8), :], f_key),
                (factors.at[pl.ds(16, 8), :], f_value), (norm, norm_out),
            )
        )
    ]
    for copy in copies:
        copy.start()
    scale = inverse[...]

    def late_start(k):
        aside, along_z, way = 1 - k // 4, (k + 1) // 2 % 2, 2 * k - 3
        return start_of(2 + aside * along_z * way, 2 + aside * (1 - along_z) * (way // 3))

    def late_copy(k, m):
        return pltpu.make_async_copy(
            late.at[k, m], outs[m].at[pl.ds(late_start(k), 2 * ROWS), :], late_sem.at[k * 3 + m]
        )

    def scale_late(k, carry):
        def scale_part(part, carry):
            at_row = pl.multiple_of(part * BLOCK, BLOCK)

            def store(m, at, value):
                late[k, m, pl.ds(at_row, BLOCK), at : at + 128] = value

            scaled(low_rows, mixes, scale, BLOCK, pl.multiple_of(late_start(k) + at_row, BLOCK), full, store)
            return carry

        lax.fori_loop(0, 2 * ROWS // BLOCK, scale_part, 0)
        for m in range(3):
            late_copy(k, m).start()
        return carry

    def wait_late(k, carry):
        for m in range(3):
            late_copy(k, m).wait()
        return carry

    lax.fori_loop(0, len(LATE), scale_late, 0)
    for copy in copies:
        copy.wait()
    lax.fori_loop(0, len(LATE), wait_late, 0)


def per_device(wq, lq, hq, wk, lk, hk, wv, lv, hv, train, step):
    any_spec = pl.BlockSpec(memory_space=pl.ANY)
    vmem = pl.BlockSpec(memory_space=pltpu.VMEM)
    f32, bf16 = jnp.float32, jnp.bfloat16
    hbm = [
        pltpu.with_memory_space_constraint(a, pltpu.HBM)
        for a in (wq, wk, wv, lq.T, lk.T, lv.T, hq, hk, hv, train.reshape(1, 32), step.reshape(1, 32))
    ]
    state = pl.pallas_call(
        gather_kernel,
        out_shape=(
            jax.ShapeDtypeStruct((24, 128), f32),
            jax.ShapeDtypeStruct((24, 128), f32),
            jax.ShapeDtypeStruct((32, 128), bf16),
            pltpu.VMEM((D_MODEL, 128), bf16),
            pltpu.VMEM((3, 128, COLS), bf16),
            pltpu.VMEM((3, D_MODEL, COLS), bf16),
        ),
        in_specs=[any_spec] * 11,
        out_specs=(vmem,) * 6,
        scratch_shapes=[
            pltpu.VMEM((2, 1, 32), f32),
            pltpu.VMEM((3, 16, 128), bf16),
            pltpu.VMEM((2, 4, 16, 16, 128), bf16),
            pltpu.VMEM((3, 16, COLS), bf16),
            pltpu.VMEM((32, 128), f32),
            pltpu.VMEM((4, 4, 8, 128), f32),
            pltpu.VMEM((32, 128), f32),
            pltpu.VMEM((4, 16, 128), f32),
            pltpu.VMEM((2, 4, 16, 128), f32),
            pltpu.SemaphoreType.DMA((11,)),
            pltpu.SemaphoreType.DMA((21,)),
            pltpu.SemaphoreType.DMA((21,)),
            pltpu.SemaphoreType.DMA((N_MESSAGES * 4,)),
            pltpu.SemaphoreType.DMA((N_MESSAGES * 4,)),
            pltpu.SemaphoreType.DMA((N_MESSAGES * 4,)),
            pltpu.SemaphoreType.DMA((N_MESSAGES * 4,)),
            pltpu.SemaphoreType.DMA,
            pltpu.SemaphoreType.DMA,
            pltpu.SemaphoreType.REGULAR,
            pltpu.SemaphoreType.REGULAR((3,)),
        ],
        compiler_params=pltpu.CompilerParams(
            collective_id=0, has_side_effects=True, vmem_limit_bytes=GATHER_LIMIT * 1024 * 1024
        ),
    )(*hbm)
    query, key, value, f_query, f_key, f_value, norm = pl.pallas_call(
        write_kernel,
        out_shape=(
            jax.ShapeDtypeStruct((D_MODEL, COLS), bf16),
            jax.ShapeDtypeStruct((D_MODEL, COLS), bf16),
            jax.ShapeDtypeStruct((D_MODEL, COLS), bf16),
            jax.ShapeDtypeStruct((8, 128), f32),
            jax.ShapeDtypeStruct((8, 128), f32),
            jax.ShapeDtypeStruct((8, 128), f32),
            jax.ShapeDtypeStruct((32, 128), bf16),
        ),
        in_specs=[vmem] * 6,
        out_specs=[any_spec] * 7,
        scratch_shapes=[
            pltpu.VMEM((len(LATE), 3, 2 * ROWS, COLS), bf16),
            pltpu.SemaphoreType.DMA((33,)),
            pltpu.SemaphoreType.DMA((len(LATE) * 3,)),
            pltpu.SemaphoreType.DMA((4,)),
        ],
        compiler_params=pltpu.CompilerParams(vmem_limit_bytes=WRITE_LIMIT * 1024 * 1024),
    )(*state)
    return (
        query, key, value,
        f_query.reshape(COLS), f_key.reshape(COLS), f_value.reshape(COLS), norm.reshape(D_MODEL),
    )


def solution(mesh):
    return jax.shard_map(
        per_device,
        mesh=mesh,
        in_specs=(
            P("zero", "model"), P("zero", None), P(None, "model"),
            P("zero", "model"), P("zero", None), P(None, "model"),
            P("zero", "model"), P("zero", None), P(None, "model"),
            P(("zero", "model")), P(("zero", "model")),
        ),
        out_specs=(
            P(None, "model"), P(None, "model"), P(None, "model"),
            P("model"), P("model"), P("model"), P(),
        ),
        check_vma=False,
    )
```

```python
import jax
import jax.numpy as jnp
from jax import lax
from jax.experimental import pallas as pl
from jax.experimental.pallas import tpu as pltpu
from jax.sharding import PartitionSpec as P

MESH = pl.DeviceIdType.MESH
D_MODEL = 4096
COLS = 1024
ROWS = 128
SUB = 32
BLOCK = 64
SIDE = 4
GATHER_LIMIT = 16
WRITE_LIMIT = 16

MESSAGES = (
    (0, 0, 0, 2, 0, 64),
    (0, 0, 1, 2, 0, 64),
    (-1, 0, 0, 1, 0, 32),
    (0, -1, 1, 2, 0, 64),
    (0, 1, 1, 2, 0, 64),
    (0, 2, 1, 2, 0, 64),
    (-1, 0, 1, 1, 0, 32),
    (-1, -1, 1, 1, 0, 32),
    (-1, 1, 1, 1, 0, 32),
    (-1, 2, 1, 1, 0, 24),
    (-1, 2, 1, 1, 24, 8),
)
N_MESSAGES = len(MESSAGES)


def scaled(low_rows, mixes, inverse, rows, start, source, store):
    low = low_rows[pl.ds(start, rows), :]
    for m in range(3):
        for pair in range(4):
            cols = slice(pair * 256, pair * 256 + 256)
            product = jnp.dot(low, mixes[m, :, cols], preferred_element_type=jnp.float32)
            for j in range(2):
                at = pair * 256 + j * 128
                row = m * 8 + pair * 2 + j
                whole = source[m, pl.ds(start, rows), at : at + 128].astype(jnp.float32) + product[:, j * 128 : j * 128 + 128]
                store(m, at, (whole * inverse[row : row + 1, :]).astype(jnp.bfloat16))


def gather_kernel(
    w_query, w_key, w_value, low_query, low_key, low_value, high_query, high_key, high_value, train, step,
    factors, inverse, norm, low_rows, mixes, full,
    gains, low_own, lows, highs, message, from_y, from_core, from_first, from_second,
    load_sem, small_send, small_recv, send_sem, recv_sem, pass_send, pass_recv, own_send, own_recv, near_sem, down_sem,
):
    zero, y = lax.axis_index("zero"), lax.axis_index("model")
    z, x, core = zero // 8, zero // 2 % 4, zero % 2
    partner = zero + 1 - 2 * core
    own = pl.multiple_of(zero * ROWS, ROWS)
    first = x + core * (z - x)
    second = z + core * (x - z)

    def index_of(z_at, x_at, core_at):
        return (z_at * 4 + x_at) * 2 + core_at

    def peer(axis, k):
        return index_of((z + axis * k) % 4, (x + (1 - axis) * k) % 4, core)

    def remote(src, dst, sems, at, target, y_at):
        return pltpu.make_async_remote_copy(
            src_ref=src, dst_ref=dst, send_sem=sems[0].at[at], recv_sem=sems[1].at[at],
            device_id=(target, y_at), device_id_type=MESH,
        )

    def upstream(at, way):
        return at // 2 if way == 1 else (at + 1) // 2 % 2

    near = [
        ((peer(0, 1), y), upstream(x, 1), 0), ((peer(0, 3), y), upstream(x, -1), 0),
        ((peer(1, 1), y), upstream(z, 1), 1), ((peer(1, 3), y), upstream(z, -1), 1),
        ((zero, (y + 1) % 4), upstream(y, 1), 2), ((zero, (y + 3) % 4), upstream(y, -1), 2),
    ]
    greeted = near + [((partner, y), 1 - core, 0)]
    n_up = sum(up for _, up, _ in greeted)

    def wait_down(group):
        n_down = sum(1 - up for _, up, at in greeted if at == group)
        pl.when(n_down > 0)(lambda: pl.semaphore_wait(down_sem.at[group], n_down))

    barrier = pltpu.get_barrier_semaphore()

    def signal(sem, device):
        pl.semaphore_signal(sem, inc=1, device_id=device, device_id_type=MESH)

    for device, up, _ in greeted:
        pl.when(up == 0)(lambda device=device: signal(barrier, device))

    small = (small_send, small_recv)
    place = second * 4 + first
    loads = [
        pltpu.make_async_copy(src, dst, load_sem.at[k])
        for k, (src, dst) in enumerate(
            (
                (w_query, full.at[0, pl.ds(own, ROWS), :]),
                (w_key, full.at[1, pl.ds(own, ROWS), :]),
                (w_value, full.at[2, pl.ds(own, ROWS), :]),
                (low_query, low_own.at[0]), (low_key, low_own.at[1]), (low_value, low_own.at[2]),
                (train, gains.at[0]), (step, gains.at[1]),
                (high_query, highs.at[0]), (high_key, highs.at[1]), (high_value, highs.at[2]),
            )
        )
    ]
    for load in loads[:3]:
        load.start()

    pl.when(n_up > 0)(lambda: pl.semaphore_wait(barrier, n_up))
    for device, up, group in greeted:
        pl.when(up == 1)(lambda device=device, group=group: signal(down_sem.at[group], device))
    for load in loads[3:]:
        load.start()
    for load in loads[:3]:
        load.wait()

    def rows_of(link, at, arriving, core_at):
        along, across, half, parts, skip, _ = MESSAGES[at]
        axis, way = link // 2, 1 - 2 * (link % 2)
        along = (along - arriving) * way
        z_at = (z + axis * along + (1 - axis) * across + 8) % 4
        x_at = (x + (1 - axis) * along + axis * across + 8) % 4
        half = axis if half == 0 else 1 - axis
        part = link % 2 if parts == 1 else 0
        return pl.multiple_of(index_of(z_at, x_at, core_at) * ROWS + half * 64 + part * SUB + skip, 8)

    def chunk_of(link, at, arriving, core_at):
        return full.at[:, pl.ds(rows_of(link, at, arriving, core_at), MESSAGES[at][5]), :]

    def link_copy(link, at, arriving=0):
        axis, way = link // 2, 1 - 2 * (link % 2)
        chunk = chunk_of(link, at, arriving, core)
        target = index_of((z + axis * way + 4) % 4, (x + (1 - axis) * way + 4) % 4, core)
        return remote(chunk, chunk, (send_sem, recv_sem), at * 4 + link, target, y)

    def pass_copy(link, at):
        chunk = chunk_of(link, at, 1, core)
        return remote(chunk, chunk, (pass_send, pass_recv), at * 4 + link, partner, y)

    def each_link(body, count=4):
        def step_of(link, carry):
            body(link)
            return carry

        lax.fori_loop(0, count, step_of, 0)

    def send(at):
        each_link(lambda link: link_copy(link, at).start())

    def arrive(at):
        def body(link):
            link_copy(link, at, 1).wait_recv()
            pass_copy(link, at).start()

        each_link(body)

    def send_first(to_up, axes):
        def body(back):
            for axis in axes:
                at = (x, z)[axis]
                up = (1 - back) * (at // 2) + back * ((at + 1) // 2 % 2)
                pl.when(up == to_up)(lambda axis=axis: link_copy(2 * axis + back, 0).start())

        each_link(body, 2)

    send_first(1, (0, 1))
    wait_down(0)
    send_first(0, (0,))
    wait_down(1)
    send_first(0, (1,))

    for load in loads[6:8]:
        load.wait()
    gain = gains[0] + gains[1]
    gain = pltpu.roll(jnp.concatenate([gain, jnp.zeros((1, 96), jnp.float32)], axis=1), 32 * y, 1)
    row = lax.broadcasted_iota(jnp.int32, (8, 128), 0)
    tile = jnp.where(row == x * 2 + core, jnp.broadcast_to(gain, (8, 128)), 0.0)
    message[24:32, :] = tile

    for load in loads[3:6] + loads[8:]:
        load.wait()
    lows[core, y, place] = low_own[y - y // 3]
    for m in range(3):
        product = lax.dot_general(
            low_own[m], highs[m], (((0,), (0,)), ((), ())), preferred_element_type=jnp.float32
        )
        value = full[m, pl.ds(own, ROWS), :].astype(jnp.float32) + 0.5 * product
        total = jnp.sum(jnp.abs(value), axis=0, keepdims=True)
        for j in range(8):
            message[m * 8 + j : m * 8 + j + 1, :] = total[:, j * 128 : (j + 1) * 128]

    core_copy = remote(message, from_core, small, 0, partner, y)
    core_copy.start()
    wait_down(2)
    for device, _, _ in near:
        signal(near_sem, device)
    pl.semaphore_wait(near_sem, 6)
    low_block = lows.at[core, y, place]
    low_first = [remote(low_block, low_block, small, 10 + k, peer(core, k), y) for k in range(1, SIDE)]
    for copy in low_first:
        copy.start()
    core_copy.wait()
    share = 1 - core
    mine = pl.ds(pl.multiple_of(share * 16, 16), 16)
    from_first[pl.ds(first, 1)] = (message[mine, :] + from_core[mine, :])[None]
    first_copies = [
        remote(from_first.at[first], from_first.at[first], small, 3 + k, peer(core, k), y)
        for k in range(1, SIDE)
    ]
    for copy in first_copies:
        copy.start()
    send(1)
    block = full.at[:, pl.ds(own, ROWS), :]
    own_copy = pltpu.make_async_remote_copy(
        src_ref=block, dst_ref=block, send_sem=own_send, recv_sem=own_recv,
        device_id=(partner, y), device_id_type=MESH,
    )
    own_copy.start()
    for m in range(3):
        mixes[m] = jnp.zeros((128, COLS), jnp.bfloat16)
        mixes[m, 16 * m : 16 * m + 16, :] = (0.5 * highs[m].astype(jnp.float32)).astype(jnp.bfloat16)

    arrive(0)
    for copy in first_copies + low_first:
        copy.wait()
    from_second[pl.ds(share, 1), pl.ds(second, 1)] = (
        from_first[0] + from_first[1] + from_first[2] + from_first[3]
    )[None, None]
    own_sum = from_second.at[share, second]
    second_copies = [remote(own_sum, own_sum, small, 6 + k, peer(1 - core, k), y) for k in range(1, SIDE)]
    low_line = lows.at[core, y, pl.ds(pl.multiple_of(second * 4, 4), 4)]
    second_copies += [remote(low_line, low_line, small, 13 + k, peer(1 - core, k), y) for k in range(1, SIDE)]
    for copy in second_copies:
        copy.start()
    send(2)
    send(3)

    arrive(1)
    send(4)
    for copy in second_copies:
        copy.wait()
    sum_copy = remote(from_second.at[share], from_second.at[share], small, 10, partner, y)
    sum_copy.start()
    low_plane = lows.at[core, y]
    low_planes = [remote(low_plane, low_plane, small, 17 + k, zero, (y + k) % 4) for k in range(1, SIDE)]
    for copy in low_planes:
        copy.start()
    sum_copy.wait()
    from_y[pl.ds(y, 1)] = from_second[1, :, 8:16, :][None]
    y_copies = [remote(from_y.at[y], from_y.at[y], small, k, zero, (y + k) % 4) for k in range(1, SIDE)]
    for copy in y_copies:
        copy.start()
    sums = [from_second[h, 0] + from_second[h, 1] + from_second[h, 2] + from_second[h, 3] for h in range(2)]
    factor = jnp.concatenate([sums[0], sums[1][:8]], axis=0) / D_MODEL
    factors[...] = factor
    inverse[...] = 1.0 / factor
    for copy in y_copies:
        copy.wait()
    for k in range(SIDE):
        rows = from_y[0, k] + from_y[1, k] + from_y[2, k] + from_y[3, k]
        norm[k * 8 : (k + 1) * 8, :] = rows.astype(jnp.bfloat16)

    for copy in low_planes:
        copy.wait()
    low_copy = remote(lows.at[core], lows.at[core], small, 17, partner, y)
    low_copy.start()
    arrive(2)
    send(5)
    low_copy.wait()
    lane = lax.broadcasted_iota(jnp.int32, (48, 128), 1)
    unit = jnp.where(lax.broadcasted_iota(jnp.int32, (48, 128), 0) == lane, 1.0, 0.0).astype(jnp.bfloat16)

    def turn(k, carry):
        core_at, major, minor = k // 16, k // 4 % 4, k % 4
        z_at = major + core_at * (minor - major)
        x_at = minor + core_at * (major - minor)
        start = pl.multiple_of(index_of(z_at, x_at, core_at) * ROWS, ROWS)
        turned = lax.dot_general(
            jnp.concatenate([lows[core_at, m, k % 16] for m in range(3)], axis=0), unit, (((0,), (0,)), ((), ())), preferred_element_type=jnp.float32
        )
        low_rows[pl.ds(start, ROWS), :] = turned.astype(jnp.bfloat16)
        return carry

    lax.fori_loop(0, 32, turn, 0)

    scale = inverse[...]

    def scale_rows(start):
        def store(m, at, value):
            full[m, pl.ds(start, 64), at : at + 128] = value

        scaled(low_rows, mixes, scale, 64, start, full, store)

    def scale_passed(at):
        def body(link):
            pass_copy(link, at).wait_recv()
            scale_rows(pl.multiple_of(rows_of(link, at, 1, 1 - core), 64))

        each_link(body)

    def scale_passed_pair(at):
        def body(axis):
            pass_copy(2 * axis, at).wait_recv()
            pass_copy(2 * axis + 1, at).wait_recv()
            scale_rows(pl.multiple_of(rows_of(2 * axis, at, 1, 1 - core), 64))

        each_link(body, 2)

    def scale_mine(at):
        def body(link):
            pass_copy(link, at).wait_send()
            scale_rows(pl.multiple_of(rows_of(link, at, 1, core), 64))

        each_link(body)

    def scale_mine_pair(at):
        def body(axis):
            pass_copy(2 * axis, at).wait_send()
            pass_copy(2 * axis + 1, at).wait_send()
            scale_rows(pl.multiple_of(rows_of(2 * axis, at, 1, core), 64))

        each_link(body, 2)

    def sent(at):
        each_link(lambda link: link_copy(link, at).wait_send())

    own_copy.wait_recv()
    each_link(lambda half: scale_rows(pl.multiple_of(partner * ROWS + half * 64, 64)), 2)
    scale_passed(0)
    sent(0)
    sent(1)
    own_copy.wait_send()
    each_link(lambda half: scale_rows(pl.multiple_of(zero * ROWS + half * 64, 64)), 2)
    arrive(3)
    send(6)
    send(7)
    scale_passed(1)
    scale_passed_pair(2)
    arrive(4)
    send(8)
    scale_passed(3)
    sent(2)
    sent(3)
    sent(4)
    scale_mine(0)
    arrive(5)
    send(9)
    send(10)
    scale_passed(4)
    sent(5)
    scale_mine_pair(2)
    arrive(6)
    sent(6)
    scale_mine(1)
    arrive(7)
    sent(7)
    scale_mine(3)
    scale_mine_pair(6)
    scale_passed_pair(6)
    sent(8)
    scale_mine(4)
    arrive(8)
    arrive(9)
    arrive(10)
    sent(9)
    sent(10)
    for at in (5, 7, 8):
        each_link(lambda link: pass_copy(link, at).wait())
    each_link(lambda link: pass_copy(link, 9).wait())
    each_link(lambda link: pass_copy(link, 10).wait())


LATE = ((2, 1), (1, 2), (3, 2), (2, 3), (2, 2))


def write_kernel(
    factors, inverse, norm, low_rows, mixes, full,
    query, key, value, f_query, f_key, f_value, norm_out, late, sem, late_sem, small_sem,
):
    zero = lax.axis_index("zero")
    z, x = zero // 8, zero // 2 % 4
    outs = (query, key, value)

    def start_of(dz, dx):
        return pl.multiple_of(((z + dz) % 4 * 4 + (x + dx) % 4) * 2 * ROWS, 2 * ROWS)

    copies = []
    for dz in range(4):
        for dx in range(4):
            if (dz, dx) not in LATE:
                for m in range(3):
                    part = pl.ds(start_of(dz, dx), 2 * ROWS)
                    copies.append(
                        pltpu.make_async_copy(full.at[m, part, :], outs[m].at[part, :], sem.at[len(copies)])
                    )
    copies += [
        pltpu.make_async_copy(src, dst, small_sem.at[k])
        for k, (src, dst) in enumerate(
            (
                (factors.at[pl.ds(0, 8), :], f_query), (factors.at[pl.ds(8, 8), :], f_key),
                (factors.at[pl.ds(16, 8), :], f_value), (norm, norm_out),
            )
        )
    ]
    for copy in copies:
        copy.start()
    scale = inverse[...]

    def late_start(k):
        aside, along_z, way = 1 - k // 4, (k + 1) // 2 % 2, 2 * k - 3
        return start_of(2 + aside * along_z * way, 2 + aside * (1 - along_z) * (way // 3))

    def late_copy(k, m):
        return pltpu.make_async_copy(
            late.at[k, m], outs[m].at[pl.ds(late_start(k), 2 * ROWS), :], late_sem.at[k * 3 + m]
        )

    def scale_late(k, carry):
        def scale_part(part, carry):
            at_row = pl.multiple_of(part * BLOCK, BLOCK)

            def store(m, at, value):
                late[k, m, pl.ds(at_row, BLOCK), at : at + 128] = value

            scaled(low_rows, mixes, scale, BLOCK, pl.multiple_of(late_start(k) + at_row, BLOCK), full, store)
            return carry

        lax.fori_loop(0, 2 * ROWS // BLOCK, scale_part, 0)
        for m in range(3):
            late_copy(k, m).start()
        return carry

    def wait_late(k, carry):
        for m in range(3):
            late_copy(k, m).wait()
        return carry

    lax.fori_loop(0, len(LATE), scale_late, 0)
    for copy in copies:
        copy.wait()
    lax.fori_loop(0, len(LATE), wait_late, 0)


def per_device(wq, lq, hq, wk, lk, hk, wv, lv, hv, train, step):
    any_spec = pl.BlockSpec(memory_space=pl.ANY)
    vmem = pl.BlockSpec(memory_space=pltpu.VMEM)
    f32, bf16 = jnp.float32, jnp.bfloat16
    hbm = [
        pltpu.with_memory_space_constraint(a, pltpu.HBM)
        for a in (wq, wk, wv, lq.T, lk.T, lv.T, hq, hk, hv, train.reshape(1, 32), step.reshape(1, 32))
    ]
    state = pl.pallas_call(
        gather_kernel,
        out_shape=(
            jax.ShapeDtypeStruct((24, 128), f32),
            jax.ShapeDtypeStruct((24, 128), f32),
            jax.ShapeDtypeStruct((32, 128), bf16),
            pltpu.VMEM((D_MODEL, 128), bf16),
            pltpu.VMEM((3, 128, COLS), bf16),
            pltpu.VMEM((3, D_MODEL, COLS), bf16),
        ),
        in_specs=[any_spec] * 11,
        out_specs=(vmem,) * 6,
        scratch_shapes=[
            pltpu.VMEM((2, 1, 32), f32),
            pltpu.VMEM((3, 16, 128), bf16),
            pltpu.VMEM((2, 4, 16, 16, 128), bf16),
            pltpu.VMEM((3, 16, COLS), bf16),
            pltpu.VMEM((32, 128), f32),
            pltpu.VMEM((4, 4, 8, 128), f32),
            pltpu.VMEM((32, 128), f32),
            pltpu.VMEM((4, 16, 128), f32),
            pltpu.VMEM((2, 4, 16, 128), f32),
            pltpu.SemaphoreType.DMA((11,)),
            pltpu.SemaphoreType.DMA((21,)),
            pltpu.SemaphoreType.DMA((21,)),
            pltpu.SemaphoreType.DMA((N_MESSAGES * 4,)),
            pltpu.SemaphoreType.DMA((N_MESSAGES * 4,)),
            pltpu.SemaphoreType.DMA((N_MESSAGES * 4,)),
            pltpu.SemaphoreType.DMA((N_MESSAGES * 4,)),
            pltpu.SemaphoreType.DMA,
            pltpu.SemaphoreType.DMA,
            pltpu.SemaphoreType.REGULAR,
            pltpu.SemaphoreType.REGULAR((3,)),
        ],
        compiler_params=pltpu.CompilerParams(
            collective_id=0, has_side_effects=True, vmem_limit_bytes=GATHER_LIMIT * 1024 * 1024
        ),
    )(*hbm)
    query, key, value, f_query, f_key, f_value, norm = pl.pallas_call(
        write_kernel,
        out_shape=(
            jax.ShapeDtypeStruct((D_MODEL, COLS), bf16),
            jax.ShapeDtypeStruct((D_MODEL, COLS), bf16),
            jax.ShapeDtypeStruct((D_MODEL, COLS), bf16),
            jax.ShapeDtypeStruct((8, 128), f32),
            jax.ShapeDtypeStruct((8, 128), f32),
            jax.ShapeDtypeStruct((8, 128), f32),
            jax.ShapeDtypeStruct((32, 128), bf16),
        ),
        in_specs=[vmem] * 6,
        out_specs=[any_spec] * 7,
        scratch_shapes=[
            pltpu.VMEM((len(LATE), 3, 2 * ROWS, COLS), bf16),
            pltpu.SemaphoreType.DMA((33,)),
            pltpu.SemaphoreType.DMA((len(LATE) * 3,)),
            pltpu.SemaphoreType.DMA((4,)),
        ],
        compiler_params=pltpu.CompilerParams(vmem_limit_bytes=WRITE_LIMIT * 1024 * 1024),
    )(*state)
    return (
        query, key, value,
        f_query.reshape(COLS), f_key.reshape(COLS), f_value.reshape(COLS), norm.reshape(D_MODEL),
    )


def solution(mesh):
    return jax.shard_map(
        per_device,
        mesh=mesh,
        in_specs=(
            P("zero", "model"), P("zero", None), P(None, "model"),
            P("zero", "model"), P("zero", None), P(None, "model"),
            P("zero", "model"), P("zero", None), P(None, "model"),
            P(("zero", "model")), P(("zero", "model")),
        ),
        out_specs=(
            P(None, "model"), P(None, "model"), P(None, "model"),
            P("model"), P("model"), P("model"), P(),
        ),
        check_vma=False,
    )
```

```python
import jax
import jax.numpy as jnp
from jax import lax
from jax.experimental import pallas as pl
from jax.experimental.pallas import tpu as pltpu
from jax.sharding import PartitionSpec as P

MESH = pl.DeviceIdType.MESH
D_MODEL = 4096
COLS = 1024
ROWS = 128
SUB = 32
BLOCK = 64
SIDE = 4
GATHER_LIMIT = 16
WRITE_LIMIT = 16

MESSAGES = (
    (0, 0, 0, 2, 0, 64),
    (0, 0, 1, 2, 0, 64),
    (-1, 0, 0, 1, 0, 32),
    (0, -1, 1, 2, 0, 64),
    (0, 1, 1, 2, 0, 64),
    (0, 2, 1, 2, 0, 64),
    (-1, 0, 1, 1, 0, 32),
    (-1, -1, 1, 1, 0, 32),
    (-1, 1, 1, 1, 0, 32),
    (-1, 2, 1, 1, 0, 24),
    (-1, 2, 1, 1, 24, 8),
)
N_MESSAGES = len(MESSAGES)


def scaled(low_rows, mixes, inverse, rows, start, source, store):
    low = low_rows[pl.ds(start, rows), :]
    for m in range(3):
        for pair in range(4):
            cols = slice(pair * 256, pair * 256 + 256)
            product = jnp.dot(low, mixes[m, :, cols], preferred_element_type=jnp.float32)
            for j in range(2):
                at = pair * 256 + j * 128
                row = m * 8 + pair * 2 + j
                whole = source[m, pl.ds(start, rows), at : at + 128].astype(jnp.float32) + product[:, j * 128 : j * 128 + 128]
                store(m, at, (whole * inverse[row : row + 1, :]).astype(jnp.bfloat16))


def gather_kernel(
    w_query, w_key, w_value, low_query, low_key, low_value, high_query, high_key, high_value, train, step,
    factors, inverse, norm, low_rows, mixes, full,
    gains, low_own, lows, highs, message, from_y, from_core, from_first, from_second,
    load_sem, small_send, small_recv, send_sem, recv_sem, pass_send, pass_recv, own_send, own_recv, near_sem, down_sem,
):
    zero, y = lax.axis_index("zero"), lax.axis_index("model")
    z, x, core = zero // 8, zero // 2 % 4, zero % 2
    partner = zero + 1 - 2 * core
    own = pl.multiple_of(zero * ROWS, ROWS)
    first = x + core * (z - x)
    second = z + core * (x - z)

    def index_of(z_at, x_at, core_at):
        return (z_at * 4 + x_at) * 2 + core_at

    def peer(axis, k):
        return index_of((z + axis * k) % 4, (x + (1 - axis) * k) % 4, core)

    def remote(src, dst, sems, at, target, y_at):
        return pltpu.make_async_remote_copy(
            src_ref=src, dst_ref=dst, send_sem=sems[0].at[at], recv_sem=sems[1].at[at],
            device_id=(target, y_at), device_id_type=MESH,
        )

    def upstream(at, way):
        return at // 2 if way == 1 else (at + 1) // 2 % 2

    near = [
        ((peer(0, 1), y), upstream(x, 1), 0), ((peer(0, 3), y), upstream(x, -1), 0),
        ((peer(1, 1), y), upstream(z, 1), 1), ((peer(1, 3), y), upstream(z, -1), 1),
        ((zero, (y + 1) % 4), upstream(y, 1), 2), ((zero, (y + 3) % 4), upstream(y, -1), 2),
    ]
    greeted = near + [((partner, y), 1 - core, 0)]
    n_up = sum(up for _, up, _ in greeted)

    def wait_down(group):
        n_down = sum(1 - up for _, up, at in greeted if at == group)
        pl.when(n_down > 0)(lambda: pl.semaphore_wait(down_sem.at[group], n_down))

    barrier = pltpu.get_barrier_semaphore()

    def signal(sem, device):
        pl.semaphore_signal(sem, inc=1, device_id=device, device_id_type=MESH)

    for device, up, _ in greeted:
        pl.when(up == 0)(lambda device=device: signal(barrier, device))

    small = (small_send, small_recv)
    place = second * 4 + first
    loads = [
        pltpu.make_async_copy(src, dst, load_sem.at[k])
        for k, (src, dst) in enumerate(
            (
                (w_query, full.at[0, pl.ds(own, ROWS), :]),
                (w_key, full.at[1, pl.ds(own, ROWS), :]),
                (w_value, full.at[2, pl.ds(own, ROWS), :]),
                (low_query, low_own.at[0]), (low_key, low_own.at[1]), (low_value, low_own.at[2]),
                (train, gains.at[0]), (step, gains.at[1]),
                (high_query, highs.at[0]), (high_key, highs.at[1]), (high_value, highs.at[2]),
            )
        )
    ]
    for load in loads[:3]:
        load.start()

    pl.when(n_up > 0)(lambda: pl.semaphore_wait(barrier, n_up))
    for device, up, group in greeted:
        pl.when(up == 1)(lambda device=device, group=group: signal(down_sem.at[group], device))
    for load in loads[3:]:
        load.start()
    for load in loads[:3]:
        load.wait()

    def rows_of(link, at, arriving, core_at):
        along, across, half, parts, skip, _ = MESSAGES[at]
        axis, way = link // 2, 1 - 2 * (link % 2)
        along = (along - arriving) * way
        z_at = (z + axis * along + (1 - axis) * across + 8) % 4
        x_at = (x + (1 - axis) * along + axis * across + 8) % 4
        half = axis if half == 0 else 1 - axis
        part = link % 2 if parts == 1 else 0
        return pl.multiple_of(index_of(z_at, x_at, core_at) * ROWS + half * 64 + part * SUB + skip, 8)

    def chunk_of(link, at, arriving, core_at):
        return full.at[:, pl.ds(rows_of(link, at, arriving, core_at), MESSAGES[at][5]), :]

    def link_copy(link, at, arriving=0):
        axis, way = link // 2, 1 - 2 * (link % 2)
        chunk = chunk_of(link, at, arriving, core)
        target = index_of((z + axis * way + 4) % 4, (x + (1 - axis) * way + 4) % 4, core)
        return remote(chunk, chunk, (send_sem, recv_sem), at * 4 + link, target, y)

    def pass_copy(link, at):
        chunk = chunk_of(link, at, 1, core)
        return remote(chunk, chunk, (pass_send, pass_recv), at * 4 + link, partner, y)

    def each_link(body, count=4):
        def step_of(link, carry):
            body(link)
            return carry

        lax.fori_loop(0, count, step_of, 0)

    def send(at):
        each_link(lambda link: link_copy(link, at).start())

    def arrive(at):
        def body(link):
            link_copy(link, at, 1).wait_recv()
            pass_copy(link, at).start()

        if at < 9:
            each_link(body)
        else:
            for link in range(4):
                body(link)

    def send_first(to_up, axes):
        def body(back):
            for axis in axes:
                at = (x, z)[axis]
                up = (1 - back) * (at // 2) + back * ((at + 1) // 2 % 2)
                pl.when(up == to_up)(lambda axis=axis: link_copy(2 * axis + back, 0).start())

        each_link(body, 2)

    send_first(1, (0, 1))
    wait_down(0)
    send_first(0, (0,))
    wait_down(1)
    send_first(0, (1,))

    for load in loads[6:8]:
        load.wait()
    gain = gains[0] + gains[1]
    gain = pltpu.roll(jnp.concatenate([gain, jnp.zeros((1, 96), jnp.float32)], axis=1), 32 * y, 1)
    row = lax.broadcasted_iota(jnp.int32, (8, 128), 0)
    tile = jnp.where(row == x * 2 + core, jnp.broadcast_to(gain, (8, 128)), 0.0)
    message[24:32, :] = tile

    for load in loads[3:6] + loads[8:]:
        load.wait()
    lows[core, y, place] = low_own[y - y // 3]
    for m in range(3):
        product = lax.dot_general(
            low_own[m], highs[m], (((0,), (0,)), ((), ())), preferred_element_type=jnp.float32
        )
        value = full[m, pl.ds(own, ROWS), :].astype(jnp.float32) + 0.5 * product
        total = jnp.sum(jnp.abs(value), axis=0, keepdims=True)
        for j in range(8):
            message[m * 8 + j : m * 8 + j + 1, :] = total[:, j * 128 : (j + 1) * 128]

    core_copy = remote(message, from_core, small, 0, partner, y)
    core_copy.start()
    wait_down(2)
    for device, _, _ in near:
        signal(near_sem, device)
    pl.semaphore_wait(near_sem, 6)
    low_block = lows.at[core, y, place]
    low_first = [remote(low_block, low_block, small, 10 + k, peer(core, k), y) for k in range(1, SIDE)]
    for copy in low_first:
        copy.start()
    core_copy.wait()
    share = 1 - core
    mine = pl.ds(pl.multiple_of(share * 16, 16), 16)
    from_first[pl.ds(first, 1)] = (message[mine, :] + from_core[mine, :])[None]
    first_copies = [
        remote(from_first.at[first], from_first.at[first], small, 3 + k, peer(core, k), y)
        for k in range(1, SIDE)
    ]
    for copy in first_copies:
        copy.start()
    send(1)
    block = full.at[:, pl.ds(own, ROWS), :]
    own_copy = pltpu.make_async_remote_copy(
        src_ref=block, dst_ref=block, send_sem=own_send, recv_sem=own_recv,
        device_id=(partner, y), device_id_type=MESH,
    )
    own_copy.start()
    for m in range(3):
        mixes[m] = jnp.zeros((128, COLS), jnp.bfloat16)
        mixes[m, 16 * m : 16 * m + 16, :] = (0.5 * highs[m].astype(jnp.float32)).astype(jnp.bfloat16)

    arrive(0)
    for copy in first_copies + low_first:
        copy.wait()
    from_second[pl.ds(share, 1), pl.ds(second, 1)] = (
        from_first[0] + from_first[1] + from_first[2] + from_first[3]
    )[None, None]
    own_sum = from_second.at[share, second]
    second_copies = [remote(own_sum, own_sum, small, 6 + k, peer(1 - core, k), y) for k in range(1, SIDE)]
    low_line = lows.at[core, y, pl.ds(pl.multiple_of(second * 4, 4), 4)]
    second_copies += [remote(low_line, low_line, small, 13 + k, peer(1 - core, k), y) for k in range(1, SIDE)]
    for copy in second_copies:
        copy.start()
    send(2)
    send(3)

    arrive(1)
    send(4)
    for copy in second_copies:
        copy.wait()
    sum_copy = remote(from_second.at[share], from_second.at[share], small, 10, partner, y)
    sum_copy.start()
    low_plane = lows.at[core, y]
    low_planes = [remote(low_plane, low_plane, small, 17 + k, zero, (y + k) % 4) for k in range(1, SIDE)]
    for copy in low_planes:
        copy.start()
    sum_copy.wait()
    from_y[pl.ds(y, 1)] = from_second[1, :, 8:16, :][None]
    y_copies = [remote(from_y.at[y], from_y.at[y], small, k, zero, (y + k) % 4) for k in range(1, SIDE)]
    for copy in y_copies:
        copy.start()
    sums = [from_second[h, 0] + from_second[h, 1] + from_second[h, 2] + from_second[h, 3] for h in range(2)]
    factor = jnp.concatenate([sums[0], sums[1][:8]], axis=0) / D_MODEL
    factors[...] = factor
    inverse[...] = 1.0 / factor
    for copy in y_copies:
        copy.wait()
    for k in range(SIDE):
        rows = from_y[0, k] + from_y[1, k] + from_y[2, k] + from_y[3, k]
        norm[k * 8 : (k + 1) * 8, :] = rows.astype(jnp.bfloat16)

    for copy in low_planes:
        copy.wait()
    low_copy = remote(lows.at[core], lows.at[core], small, 17, partner, y)
    low_copy.start()
    arrive(2)
    send(5)
    low_copy.wait()
    lane = lax.broadcasted_iota(jnp.int32, (48, 128), 1)
    unit = jnp.where(lax.broadcasted_iota(jnp.int32, (48, 128), 0) == lane, 1.0, 0.0).astype(jnp.bfloat16)

    def turn(k, carry):
        core_at, major, minor = k // 16, k // 4 % 4, k % 4
        z_at = major + core_at * (minor - major)
        x_at = minor + core_at * (major - minor)
        start = pl.multiple_of(index_of(z_at, x_at, core_at) * ROWS, ROWS)
        turned = lax.dot_general(
            jnp.concatenate([lows[core_at, m, k % 16] for m in range(3)], axis=0), unit, (((0,), (0,)), ((), ())), preferred_element_type=jnp.float32
        )
        low_rows[pl.ds(start, ROWS), :] = turned.astype(jnp.bfloat16)
        return carry

    lax.fori_loop(0, 32, turn, 0)

    scale = inverse[...]

    def scale_rows(start):
        def store(m, at, value):
            full[m, pl.ds(start, 64), at : at + 128] = value

        scaled(low_rows, mixes, scale, 64, start, full, store)

    def scale_passed(at):
        def body(link):
            pass_copy(link, at).wait_recv()
            scale_rows(pl.multiple_of(rows_of(link, at, 1, 1 - core), 64))

        each_link(body)

    def scale_passed_pair(at):
        def body(axis):
            pass_copy(2 * axis, at).wait_recv()
            pass_copy(2 * axis + 1, at).wait_recv()
            scale_rows(pl.multiple_of(rows_of(2 * axis, at, 1, 1 - core), 64))

        each_link(body, 2)

    def scale_mine(at):
        def body(link):
            pass_copy(link, at).wait_send()
            scale_rows(pl.multiple_of(rows_of(link, at, 1, core), 64))

        each_link(body)

    def scale_mine_pair(at):
        def body(axis):
            pass_copy(2 * axis, at).wait_send()
            pass_copy(2 * axis + 1, at).wait_send()
            scale_rows(pl.multiple_of(rows_of(2 * axis, at, 1, core), 64))

        each_link(body, 2)

    def sent(at):
        each_link(lambda link: link_copy(link, at).wait_send())

    own_copy.wait_recv()
    each_link(lambda half: scale_rows(pl.multiple_of(partner * ROWS + half * 64, 64)), 2)
    scale_passed(0)
    sent(0)
    sent(1)
    own_copy.wait_send()
    each_link(lambda half: scale_rows(pl.multiple_of(zero * ROWS + half * 64, 64)), 2)
    arrive(3)
    send(6)
    send(7)
    scale_passed(1)
    scale_passed_pair(2)
    arrive(4)
    send(8)
    scale_passed(3)
    sent(2)
    sent(3)
    sent(4)
    scale_mine(0)
    arrive(5)
    send(9)
    send(10)
    scale_passed(4)
    sent(5)
    scale_mine_pair(2)
    arrive(6)
    sent(6)
    scale_mine(1)
    arrive(7)
    sent(7)
    scale_mine(3)
    scale_mine_pair(6)
    scale_passed_pair(6)
    sent(8)
    scale_mine(4)
    arrive(8)
    for at in (5, 7, 8):
        each_link(lambda link: pass_copy(link, at).wait())
    arrive(9)
    arrive(10)
    sent(9)
    sent(10)
    each_link(lambda link: pass_copy(link, 9).wait())
    each_link(lambda link: pass_copy(link, 10).wait())


LATE = ((2, 1), (1, 2), (3, 2), (2, 3), (2, 2))


def write_kernel(
    factors, inverse, norm, low_rows, mixes, full,
    query, key, value, f_query, f_key, f_value, norm_out, late, sem, late_sem, small_sem,
):
    zero = lax.axis_index("zero")
    z, x = zero // 8, zero // 2 % 4
    outs = (query, key, value)

    def start_of(dz, dx):
        return pl.multiple_of(((z + dz) % 4 * 4 + (x + dx) % 4) * 2 * ROWS, 2 * ROWS)

    copies = []
    for dz in range(4):
        for dx in range(4):
            if (dz, dx) not in LATE:
                for m in range(3):
                    part = pl.ds(start_of(dz, dx), 2 * ROWS)
                    copies.append(
                        pltpu.make_async_copy(full.at[m, part, :], outs[m].at[part, :], sem.at[len(copies)])
                    )
    copies += [
        pltpu.make_async_copy(src, dst, small_sem.at[k])
        for k, (src, dst) in enumerate(
            (
                (factors.at[pl.ds(0, 8), :], f_query), (factors.at[pl.ds(8, 8), :], f_key),
                (factors.at[pl.ds(16, 8), :], f_value), (norm, norm_out),
            )
        )
    ]
    for copy in copies:
        copy.start()
    scale = inverse[...]

    def late_start(k):
        aside, along_z, way = 1 - k // 4, (k + 1) // 2 % 2, 2 * k - 3
        return start_of(2 + aside * along_z * way, 2 + aside * (1 - along_z) * (way // 3))

    def late_copy(k, m):
        return pltpu.make_async_copy(
            late.at[k, m], outs[m].at[pl.ds(late_start(k), 2 * ROWS), :], late_sem.at[k * 3 + m]
        )

    def scale_late(k, carry):
        def scale_part(part, carry):
            at_row = pl.multiple_of(part * BLOCK, BLOCK)

            def store(m, at, value):
                late[k, m, pl.ds(at_row, BLOCK), at : at + 128] = value

            scaled(low_rows, mixes, scale, BLOCK, pl.multiple_of(late_start(k) + at_row, BLOCK), full, store)
            return carry

        lax.fori_loop(0, 2 * ROWS // BLOCK, scale_part, 0)
        for m in range(3):
            late_copy(k, m).start()
        return carry

    def wait_late(k, carry):
        for m in range(3):
            late_copy(k, m).wait()
        return carry

    lax.fori_loop(0, len(LATE), scale_late, 0)
    for copy in copies:
        copy.wait()
    lax.fori_loop(0, len(LATE), wait_late, 0)


def per_device(wq, lq, hq, wk, lk, hk, wv, lv, hv, train, step):
    any_spec = pl.BlockSpec(memory_space=pl.ANY)
    vmem = pl.BlockSpec(memory_space=pltpu.VMEM)
    f32, bf16 = jnp.float32, jnp.bfloat16
    hbm = [
        pltpu.with_memory_space_constraint(a, pltpu.HBM)
        for a in (wq, wk, wv, lq.T, lk.T, lv.T, hq, hk, hv, train.reshape(1, 32), step.reshape(1, 32))
    ]
    state = pl.pallas_call(
        gather_kernel,
        out_shape=(
            jax.ShapeDtypeStruct((24, 128), f32),
            jax.ShapeDtypeStruct((24, 128), f32),
            jax.ShapeDtypeStruct((32, 128), bf16),
            pltpu.VMEM((D_MODEL, 128), bf16),
            pltpu.VMEM((3, 128, COLS), bf16),
            pltpu.VMEM((3, D_MODEL, COLS), bf16),
        ),
        in_specs=[any_spec] * 11,
        out_specs=(vmem,) * 6,
        scratch_shapes=[
            pltpu.VMEM((2, 1, 32), f32),
            pltpu.VMEM((3, 16, 128), bf16),
            pltpu.VMEM((2, 4, 16, 16, 128), bf16),
            pltpu.VMEM((3, 16, COLS), bf16),
            pltpu.VMEM((32, 128), f32),
            pltpu.VMEM((4, 4, 8, 128), f32),
            pltpu.VMEM((32, 128), f32),
            pltpu.VMEM((4, 16, 128), f32),
            pltpu.VMEM((2, 4, 16, 128), f32),
            pltpu.SemaphoreType.DMA((11,)),
            pltpu.SemaphoreType.DMA((21,)),
            pltpu.SemaphoreType.DMA((21,)),
            pltpu.SemaphoreType.DMA((N_MESSAGES * 4,)),
            pltpu.SemaphoreType.DMA((N_MESSAGES * 4,)),
            pltpu.SemaphoreType.DMA((N_MESSAGES * 4,)),
            pltpu.SemaphoreType.DMA((N_MESSAGES * 4,)),
            pltpu.SemaphoreType.DMA,
            pltpu.SemaphoreType.DMA,
            pltpu.SemaphoreType.REGULAR,
            pltpu.SemaphoreType.REGULAR((3,)),
        ],
        compiler_params=pltpu.CompilerParams(
            collective_id=0, has_side_effects=True, vmem_limit_bytes=GATHER_LIMIT * 1024 * 1024
        ),
    )(*hbm)
    query, key, value, f_query, f_key, f_value, norm = pl.pallas_call(
        write_kernel,
        out_shape=(
            jax.ShapeDtypeStruct((D_MODEL, COLS), bf16),
            jax.ShapeDtypeStruct((D_MODEL, COLS), bf16),
            jax.ShapeDtypeStruct((D_MODEL, COLS), bf16),
            jax.ShapeDtypeStruct((8, 128), f32),
            jax.ShapeDtypeStruct((8, 128), f32),
            jax.ShapeDtypeStruct((8, 128), f32),
            jax.ShapeDtypeStruct((32, 128), bf16),
        ),
        in_specs=[vmem] * 6,
        out_specs=[any_spec] * 7,
        scratch_shapes=[
            pltpu.VMEM((len(LATE), 3, 2 * ROWS, COLS), bf16),
            pltpu.SemaphoreType.DMA((33,)),
            pltpu.SemaphoreType.DMA((len(LATE) * 3,)),
            pltpu.SemaphoreType.DMA((4,)),
        ],
        compiler_params=pltpu.CompilerParams(vmem_limit_bytes=WRITE_LIMIT * 1024 * 1024),
    )(*state)
    return (
        query, key, value,
        f_query.reshape(COLS), f_key.reshape(COLS), f_value.reshape(COLS), norm.reshape(D_MODEL),
    )


def solution(mesh):
    return jax.shard_map(
        per_device,
        mesh=mesh,
        in_specs=(
            P("zero", "model"), P("zero", None), P(None, "model"),
            P("zero", "model"), P("zero", None), P(None, "model"),
            P("zero", "model"), P("zero", None), P(None, "model"),
            P(("zero", "model")), P(("zero", "model")),
        ),
        out_specs=(
            P(None, "model"), P(None, "model"), P(None, "model"),
            P("model"), P("model"), P("model"), P(),
        ),
        check_vma=False,
    )
```
